32 devices in a mesh: tp: 4 (over z), fsdp: 8 (over y, x, core).
Axes of the slice: x: 2, y: 2, z: 4, core: 2. Of those that a mesh axis runs over, the one named last changes fastest.
Arguments:
- x_in: bfloat16 [24, 768, 2048], P('fsdp')
- dy_out: bfloat16 [24, 768, 2048], P('fsdp')
- ln_gain: float32 [2048], P('fsdp')
- w_q: bfloat16 [2048, 2048], P('fsdp', 'tp')
- w_k: bfloat16 [2048, 256], P('fsdp')
- w_v: bfloat16 [2048, 256], P('fsdp')
- w_o: bfloat16 [2048, 2048], P('tp', 'fsdp')
- w_gate: bfloat16 [2048, 8192], P('fsdp', 'tp')
- w_up: bfloat16 [2048, 8192], P('fsdp', 'tp')
- w_down: bfloat16 [8192, 2048], P('tp', 'fsdp')
Outputs:
- output 1: bfloat16 [24, 768, 2048], P('fsdp')
- output 2: bfloat16 [24, 768, 2048], P('fsdp')
- output 3: float32 [2048], P('fsdp')
- output 4: float32 [2048, 2048], P('fsdp', 'tp')
- output 5: float32 [2048, 256], P('fsdp')
- output 6: float32 [2048, 256], P('fsdp')
- output 7: float32 [2048, 2048], P('tp', 'fsdp')
- output 8: float32 [2048, 8192], P('fsdp', 'tp')
- output 9: float32 [2048, 8192], P('fsdp', 'tp')
- output 10: float32 [8192, 2048], P('tp', 'fsdp')
All inputs are finite; a program needn't handle non-finite values.
Results may differ from the reference program's by a relative error of at most 0.0152999.
Values are sent between devices in bfloat16 or wider.
A program may use at most 1 GiB of HBM per device.

```python
import math
import jax
import jax.numpy as jnp
from jax import lax

D_MODEL = 2048
N_HEADS = 8
HEAD_DIM = 256
D_FF = 8192
N_BATCH = 24
SEQ_LEN = 768


def setup_inputs(seed: int = 0) -> dict:
    keys = jax.random.split(jax.random.key(seed), 10)
    inner = N_HEADS * HEAD_DIM
    scale_model = 1.0 / math.sqrt(D_MODEL)

    def draw_normal(slot, shape, scale):
        return (jax.random.normal(keys[slot], shape, jnp.float32) * scale).astype(jnp.bfloat16)

    return {
        'x_in': draw_normal(0, (N_BATCH, SEQ_LEN, D_MODEL), 1.0),
        'dy_out': draw_normal(1, (N_BATCH, SEQ_LEN, D_MODEL), 1.0),
        'ln_gain': jax.random.uniform(keys[2], (D_MODEL,), jnp.float32, 0.5, 1.5),
        'w_q': draw_normal(3, (D_MODEL, inner), scale_model),
        'w_k': draw_normal(4, (D_MODEL, HEAD_DIM), scale_model),
        'w_v': draw_normal(5, (D_MODEL, HEAD_DIM), scale_model),
        'w_o': draw_normal(6, (inner, D_MODEL), 1.0 / math.sqrt(inner)),
        'w_gate': draw_normal(7, (D_MODEL, D_FF), scale_model),
        'w_up': draw_normal(8, (D_MODEL, D_FF), scale_model),
        'w_down': draw_normal(9, (D_FF, D_MODEL), 1.0 / math.sqrt(D_FF)),
    }


def to_bf16(vals):
    return vals.astype(jnp.bfloat16).astype(jnp.float32)


def layer_norm(x_f32, gain):
    x_mean = jnp.mean(x_f32, axis=-1, keepdims=True)
    x_cent = x_f32 - x_mean
    x_var = jnp.mean(x_cent * x_cent, axis=-1, keepdims=True)
    return to_bf16(x_cent * lax.rsqrt(x_var + 1e-5) * gain)


def rope_tables():
    half_dim = HEAD_DIM // 2
    inv_freq = jnp.power(10000.0, -2.0 * jnp.arange(half_dim, dtype=jnp.float32) / HEAD_DIM)
    angle = jnp.arange(SEQ_LEN, dtype=jnp.float32)[:, None] * inv_freq[None, :]
    return jnp.cos(angle), jnp.sin(angle)


def rotate(vals, cos_t, sin_t):
    half_dim = vals.shape[-1] // 2
    first = vals[..., :half_dim]
    second = vals[..., half_dim:]
    return jnp.concatenate([first * cos_t - second * sin_t, second * cos_t + first * sin_t], axis=-1)


def attend_rows(q_rot, k_rot, v_val):
    causal = lax.broadcasted_iota(jnp.int32, (SEQ_LEN, SEQ_LEN), 0) >= lax.broadcasted_iota(jnp.int32, (SEQ_LEN, SEQ_LEN), 1)

    def one_head(q_head, k_row, v_row):
        scores = jnp.dot(q_head, k_row.T, preferred_element_type=jnp.float32)
        scores = jnp.where(causal, scores, -1e30)
        row_max = lax.stop_gradient(jnp.max(scores, axis=-1, keepdims=True))
        exp_val = jnp.exp(scores - row_max)
        att_prob = to_bf16(exp_val / jnp.sum(exp_val, axis=-1, keepdims=True))
        return to_bf16(jnp.dot(att_prob, v_row, preferred_element_type=jnp.float32))

    head_step = jax.checkpoint(one_head)

    def one_row(row):
        q_row, k_row, v_row = row

        def per_head(q_head):
            return head_step(q_head, k_row, v_row)

        head_outs = lax.map(per_head, jnp.swapaxes(q_row, 0, 1))
        return jnp.swapaxes(head_outs, 0, 1)

    return lax.map(one_row, (q_rot, k_rot, v_val))


def layer_forward(x_f32, gain, w_q, w_k, w_v, w_o, w_gate, w_up, w_down):
    n_batch = x_f32.shape[0]
    h_norm = layer_norm(x_f32, gain)
    q_raw = to_bf16(jnp.einsum('bsd,de->bse', h_norm, w_q))
    k_raw = to_bf16(jnp.einsum('bsd,de->bse', h_norm, w_k))
    v_val = to_bf16(jnp.einsum('bsd,de->bse', h_norm, w_v))
    gate_val = to_bf16(jnp.einsum('bsd,df->bsf', h_norm, w_gate))
    up_val = to_bf16(jnp.einsum('bsd,df->bsf', h_norm, w_up))
    cos_t, sin_t = rope_tables()
    q_heads = q_raw.reshape(n_batch, SEQ_LEN, N_HEADS, HEAD_DIM)
    q_rot = to_bf16(rotate(q_heads, cos_t[:, None, :], sin_t[:, None, :]) * (1.0 / math.sqrt(HEAD_DIM)))
    k_rot = to_bf16(rotate(k_raw, cos_t, sin_t))
    att_out = attend_rows(q_rot, k_rot, v_val).reshape(n_batch, SEQ_LEN, N_HEADS * HEAD_DIM)
    mlp_act = to_bf16(jax.nn.silu(gate_val) * up_val)
    branch = jnp.einsum('bse,ed->bsd', att_out, w_o) + jnp.einsum('bsf,fd->bsd', mlp_act, w_down)
    return x_f32 + branch


def reference(x_in, dy_out, ln_gain, w_q, w_k, w_v, w_o, w_gate, w_up, w_down):
    y_f32, pullback = jax.vjp(layer_forward, x_in.astype(jnp.float32), ln_gain, w_q.astype(jnp.float32), w_k.astype(jnp.float32), w_v.astype(jnp.float32), w_o.astype(jnp.float32), w_gate.astype(jnp.float32), w_up.astype(jnp.float32), w_down.astype(jnp.float32))
    gradients = pullback(dy_out.astype(jnp.float32))
    return (y_f32.astype(jnp.bfloat16), gradients[0].astype(jnp.bfloat16), gradients[1], gradients[2], gradients[3], gradients[4], gradients[5], gradients[6], gradients[7], gradients[8])
```

```python
import functools
import math
import jax
import jax.numpy as jnp
from jax import lax
from jax.experimental import pallas as pl
from jax.experimental.pallas import tpu as pltpu
from jax.sharding import PartitionSpec as P


F32 = jnp.float32
BF16 = jnp.bfloat16
WIRE = jnp.bfloat16


def mm(form, left, right):
    return jnp.einsum(form, left, right, preferred_element_type=F32)


def layer_norm(x_f32, gain):
    x_mean = jnp.mean(x_f32, axis=-1, keepdims=True)
    x_cent = x_f32 - x_mean
    x_var = jnp.mean(x_cent * x_cent, axis=-1, keepdims=True)
    return (x_cent * lax.rsqrt(x_var + 1e-5) * gain).astype(BF16)


def rope_tables(seq_len, head_dim):
    half_dim = head_dim // 2
    inv_freq = jnp.power(10000.0, -2.0 * jnp.arange(half_dim, dtype=F32) / head_dim)
    angle = jnp.arange(seq_len, dtype=F32)[:, None] * inv_freq[None, :]
    return jnp.cos(angle), jnp.sin(angle)


def rotate(vals, cos_t, sin_t):
    half_dim = vals.shape[-1] // 2
    first = vals[..., :half_dim]
    second = vals[..., half_dim:]
    return jnp.concatenate([first * cos_t - second * sin_t, second * cos_t + first * sin_t], axis=-1)


def attend(q_rot, k_rot, v_val):
    seq_len = q_rot.shape[1]
    causal = lax.broadcasted_iota(jnp.int32, (seq_len, 1, seq_len), 0) >= lax.broadcasted_iota(jnp.int32, (seq_len, 1, seq_len), 2)
    scores = jnp.einsum('crie,cle->cril', q_rot, k_rot, preferred_element_type=F32)
    scores = jnp.where(causal, scores, -1e30)
    row_max = lax.stop_gradient(jnp.max(scores, axis=-1, keepdims=True))
    exp_val = jnp.exp(scores - row_max)
    att_prob = (exp_val / jnp.sum(exp_val, axis=-1, keepdims=True)).astype(BF16)
    return jnp.einsum('cril,cle->crie', att_prob, v_val, preferred_element_type=F32).astype(BF16)


def swiglu(gate_val, up_val):
    return (jax.nn.silu(gate_val.astype(F32)) * up_val.astype(F32)).astype(BF16)


def gather(part, axis):
    return lax.all_gather(part, 'fsdp', axis=axis, tiled=True)


def scatter(grad, axis):
    return lax.psum_scatter(grad, 'fsdp', scatter_dimension=axis, tiled=True)


def after(val, *others):
    return lax.optimization_barrier((val,) + others)[0]


def line_sum(val, z, step):
    order = (0, 1, 2) if step > 0 else (3, 2, 1)
    msg = val
    got = None
    for i in order:
        if got is not None:
            msg = (val.astype(F32) + got.astype(F32)).astype(BF16)
        got = lax.ppermute(msg, 'tp', [(i, i + step)])
    return got


def row_loop(rows, step, fn):
    def body(i, carry):
        fn(pl.ds(pl.multiple_of(i * step, step), step))
        return carry

    lax.fori_loop(0, rows // step, body, 0)


def contract(left, right, dims):
    return lax.dot_general(left, right, ((dims[:1], dims[1:]), ((), ())), preferred_element_type=F32)


def back_kernel(dims, acat, wod, gate, up, dact, dq, wcat, h, dy, x, dhkv, gain,
                part, out, line, dcat, peer_a, peer_b, own_a, own_b, got_a, got_b, gsum,
                wa, wb, ctile, ytile, gt, ut, dt, ot, rt, sa, sb, zr, zo, zs, zx, zd, zk, gv,
                load, wload, wait_y, zload, zstore, rs_s, rs_r, ag_s, ag_r, core_s, core_r, far_s, far_r, own_s):
    nc, cr, col, tile = dims
    tok, width = h.shape
    ka, kb = acat.shape[1], wcat.shape[1]
    ff = gate.shape[1]
    rt_rows = 2 * cr
    blk = width // 8
    mid = width // 2
    na, nb = ka // tile, kb // tile
    me = lax.axis_index('fsdp')
    z = lax.axis_index('tp')
    last = 3

    def remote(src, dst, send, recv, **to):
        return pltpu.make_async_remote_copy(src_ref=src, dst_ref=dst, send_sem=send, recv_sem=recv,
                                            device_id=to, device_id_type=pl.DeviceIdType.MESH)

    def local(src, dst, sem):
        return pltpu.make_async_copy(src, dst, sem)

    def chunk_rows(d, c):
        return pl.ds(pl.multiple_of(lax.rem(c, nc) * rt_rows + d * cr, cr), cr)

    def slot(t):
        for d in range(2):
            rank = z if d == 0 else last - z
            up_z, down_z = lax.rem(z + 1, last + 1), lax.rem(z + last, last + 1)
            fwd, back = (up_z, down_z) if d == 0 else (down_z, up_z)

            def hop(c):
                return remote(part.at[lax.div(c, nc), chunk_rows(d, c)], line.at[d, c], rs_s.at[d, c], rs_r.at[d, c], tp=fwd)

            def mid_hop(c):
                return remote(zs.at[d, lax.rem(c, 2)], line.at[d, c], rs_s.at[d, c], rs_r.at[d, c], tp=fwd)

            def first_bcast(c):
                return remote(zs.at[d, lax.rem(c, 2)], out.at[lax.div(c, nc), chunk_rows(d, c)], ag_s.at[d, c], ag_r.at[d, c], tp=back)

            def bcast(c):
                rows = chunk_rows(d, c)
                return remote(out.at[lax.div(c, nc), rows], out.at[lax.div(c, nc), rows], ag_s.at[d, c], ag_r.at[d, c], tp=back)

            def keep(c):
                return local(zs.at[d, lax.rem(c, 2)], out.at[lax.div(c, nc), chunk_rows(d, c)], zstore.at[d, lax.rem(c, 2)])

            @pl.when((rank == 0) & (t >= 0) & (t < 2 * nc))
            def _():
                hop(t).start()

            c = t - rank

            @pl.when((rank > 0) & (c >= 0) & (c < 2 * nc))
            def _():
                rows = chunk_rows(d, c)
                mine = local(part.at[lax.div(c, nc), rows], zo, zload.at[0])
                mine.start()
                hop(c).wait_recv()
                theirs = local(line.at[d, c], zr, zload.at[1])
                theirs.start()

                @pl.when(rank < last)
                def _():
                    @pl.when(c >= 2)
                    def _():
                        mid_hop(c - 2).wait_send()

                    mine.wait()
                    theirs.wait()

                    def add(sl):
                        zs[d, lax.rem(c, 2), sl, :] = (zr[sl, :].astype(F32) + zo[sl, :].astype(F32)).astype(BF16)

                    row_loop(cr, 16, add)
                    mid_hop(c).start()

                @pl.when(rank == last)
                def _():
                    xs = local(x.at[rows], zx, zload.at[2])
                    ds = local(dy.at[rows], zd, zload.at[3])
                    ks = local(dhkv.at[pl.ds(pl.multiple_of(lax.rem(c, nc) * cr, cr), cr)], zk, zload.at[4])
                    xs.start()
                    ds.start()
                    ks.start()

                    @pl.when(c >= 2)
                    def _():
                        first_bcast(c - 2).wait_send()
                        keep(c - 2).wait()

                    mine.wait()
                    theirs.wait()
                    xs.wait()
                    ds.wait()
                    ks.wait()

                    @pl.when(c < nc)
                    def _():
                        def fin(sl):
                            branch = zr[sl, :].astype(F32) + zo[sl, :].astype(F32)
                            zs[d, lax.rem(c, 2), sl, :] = (zx[sl, :].astype(F32) + branch).astype(BF16)

                        row_loop(cr, 16, fin)

                    @pl.when(c >= nc)
                    def _():
                        def fin(sl):
                            dh = (zr[sl, :].astype(F32) + zo[sl, :].astype(F32) + zk[sl, :]).astype(BF16).astype(F32)
                            xv = zx[sl, :].astype(F32)
                            cent = xv - jnp.mean(xv, axis=-1, keepdims=True)
                            inv = lax.rsqrt(jnp.mean(cent * cent, axis=-1, keepdims=True) + 1e-5)
                            hat = cent * inv
                            gv[8:9, :] = gv[8:9, :] + jnp.sum(dh * hat, axis=0, keepdims=True)
                            dn = dh * gv[0:1, :]
                            dx = inv * (dn - jnp.mean(dn, axis=-1, keepdims=True)
                                        - hat * jnp.mean(dn * hat, axis=-1, keepdims=True))
                            zs[d, lax.rem(c, 2), sl, :] = (zd[sl, :].astype(F32) + dx).astype(BF16)

                        row_loop(cr, 16, fin)

                    keep(c).start()
                    first_bcast(c).start()

            e = t - (last + 1) - (2 - rank)

            @pl.when(((rank == 1) | (rank == 2)) & (e >= 0) & (e < 2 * nc))
            def _():
                bcast(e).wait_recv()
                bcast(e).start()

            @pl.when(t == 2 * nc + 4)
            def _():
                def each(c, carry):
                    @pl.when(rank == 0)
                    def _():
                        hop(c).wait_send()
                        bcast(c).wait_recv()

                    @pl.when((rank == 1) | (rank == 2))
                    def _():
                        bcast(c).wait_send()

                        @pl.when(c >= 2 * nc - 2)
                        def _():
                            mid_hop(c).wait_send()

                    @pl.when((rank == last) & (c >= 2 * nc - 2))
                    def _():
                        first_bcast(c).wait_send()
                        keep(c).wait()

                    return carry

                lax.fori_loop(0, 2 * nc, each, 0)

    def tile_rows(k):
        return pl.ds(pl.multiple_of(k * rt_rows, rt_rows), rt_rows)

    def y_step(k):
        src = local(acat.at[tile_rows(k)], ctile.at[:, pl.ds(0, ka)], load.at[0])
        src.start()
        src.wait()

        def cols(j, carry):
            cs = pl.ds(pl.multiple_of(j * col, col), col)
            ytile[:, cs] = contract(ctile[:, 0:ka], wa[0:ka, cs], (1, 0)).astype(BF16)
            return carry

        lax.fori_loop(0, width // col, cols, 0)
        dst = local(ytile, part.at[0, tile_rows(k)], wait_y)
        dst.start()
        dst.wait()

    def h_step(k):
        rows = tile_rows(k)
        srcs = [local(gate.at[rows], gt, load.at[0]), local(up.at[rows], ut, load.at[1]),
                local(dact.at[rows], dt, load.at[2]), local(dq.at[rows], ctile.at[:, pl.ds(2 * ff, kb - 2 * ff)], load.at[3])]
        for s in srcs:
            s.start()
        for s in srcs:
            s.wait()

        def act_back(sl):
            g = gt[sl, :].astype(F32)
            d_act = dt[sl, :].astype(F32)
            sig = jax.nn.sigmoid(g)
            ctile[sl, 0:ff] = (d_act * ut[sl, :].astype(F32) * (sig + g * sig * (1.0 - sig))).astype(BF16)
            ctile[sl, ff:2 * ff] = (d_act * (g * sig)).astype(BF16)

        row_loop(rt_rows, 16, act_back)
        keep = local(ctile, dcat.at[rows], load.at[4])
        keep.start()

        def cols(j, carry):
            cs = pl.ds(pl.multiple_of(j * col, col), col)
            ytile[:, cs] = contract(ctile[...], wb[cs, 0:kb], (1, 1)).astype(BF16)
            return carry

        lax.fori_loop(0, width // col, cols, 0)
        dst = local(ytile, part.at[1, rows], wait_y)
        dst.start()
        dst.wait()
        keep.wait()

    def out_weights():
        return local(wod, wa.at[pl.ds(0, ka)], wload.at[0])

    def in_weights():
        return local(wcat, wb.at[pl.ds(0, width), pl.ds(0, kb)], wload.at[1])

    def operands(src, wide):
        cps = [local(wide, wb.at[pl.ds(0, tok), pl.ds(0, wide.shape[1])], wload.at[8])]
        for q in range(8):
            mask = 2 * (q % 4) + q // 4
            cols = pl.ds(pl.multiple_of((me ^ mask) * blk, blk), blk)
            cps.append(local(src.at[:, cols], wa.at[pl.ds(0, tok), pl.ds(q * blk, blk)], wload.at[q]))
        for c in cps:
            c.start()
        for c in cps:
            c.wait()

    def prod(is_a, k, odd):
        cs = pl.ds(pl.multiple_of(k * tile, tile), tile)
        half = pl.ds(odd * mid, mid)
        if is_a:
            return contract(wb[0:tok, cs], wa[0:tok, half], (0, 0))
        return contract(wa[0:tok, half], wb[0:tok, cs], (0, 0))

    def place(ref, is_a, k):
        par = pl.multiple_of(lax.rem(k, 2) * tile, tile)
        return ref.at[pl.ds(par, tile), :] if is_a else ref.at[:, pl.ds(par, tile)]

    def whole(ref, is_a, k):
        cs = pl.ds(pl.multiple_of(k * tile, tile), tile)
        return ref.at[cs, :] if is_a else ref.at[:, cs]

    def piece(ref, is_a, q):
        return ref.at[:, pl.ds(q * blk, blk)] if is_a else ref.at[pl.ds(q * blk, blk), :]

    def odd_steps(is_a, lo, hi):
        base = 0 if is_a else na
        peer = peer_a if is_a else peer_b

        def send(k):
            return remote(place(ot, is_a, k), whole(peer, is_a, k), core_s.at[base + k], core_r.at[base + k], fsdp=me ^ 1)

        n = na if is_a else nb

        def one(k, carry):
            @pl.when(k >= 2)
            def _():
                send(k - 2).wait_send()

            place(ot, is_a, k)[...] = prod(is_a, k, 1)
            send(k).start()

            @pl.when(k == n - 1)
            def _():
                send(k - 1).wait_send()
                send(k).wait_send()

            return carry

        lax.fori_loop(lo, hi, one, 0)

    def even_steps(is_a, lo, hi):
        base = 0 if is_a else na
        peer, own, got = (peer_a, own_a, got_a) if is_a else (peer_b, own_b, got_b)
        stage = sa if is_a else sb
        n = na if is_a else nb

        def take(k):
            return remote(place(ot, is_a, k), whole(peer, is_a, k), core_s.at[base + k], core_r.at[base + k], fsdp=me ^ 1)

        def fetch(k):
            return local(whole(peer, is_a, k), place(rt, is_a, 0), own_s.at[2])

        def mine(k):
            return local(piece(place(ot, is_a, k), is_a, 0), whole(own, is_a, k), own_s.at[lax.rem(k, 2)])

        def away(k, q):
            return remote(stage.at[lax.rem(k, 2), q], whole(got.at[q], is_a, k), far_s.at[q, base + k], far_r.at[q, base + k],
                          fsdp=me ^ (2 * (q + 1)))

        def drain(k):
            mine(k).wait()
            for q in range(3):
                away(k, q).wait_send()

        def one(k, carry):
            take(k).wait_recv()
            fetch(k).start()

            @pl.when(k >= 2)
            def _():
                drain(k - 2)

            fetch(k).wait()
            place(ot, is_a, k)[...] = prod(is_a, k, 0) + place(rt, is_a, 0)[...]
            mine(k).start()
            for q in range(3):
                stage[lax.rem(k, 2), q] = piece(place(ot, is_a, k), is_a, q + 1)[...].astype(WIRE)
                away(k, q).start()

            @pl.when(k == n - 1)
            def _():
                drain(k - 1)
                drain(k)

            return carry

        lax.fori_loop(lo, hi, one, 0)

    def far_waits(is_a):
        base = 0 if is_a else na
        got = got_a if is_a else got_b
        stage = sa if is_a else sb

        def one(k, carry):
            for q in range(3):
                remote(stage.at[0, q], whole(got.at[q], is_a, k), far_s.at[q, base + k], far_r.at[q, base + k],
                       fsdp=me ^ (2 * (q + 1))).wait_recv()
            return carry

        lax.fori_loop(0, na if is_a else nb, one, 0)

    out_weights().start()
    in_weights().start()
    gv[8:16, :] = jnp.zeros((8, width), F32)
    first = local(gain, gv.at[pl.ds(0, 8)], load.at[0])
    first.start()
    first.wait()
    half_b = (nb + 1) // 2

    def step(s, carry):
        slot(s - 1)

        @pl.when(s < nc)
        def _():
            @pl.when(s == 0)
            def _():
                out_weights().wait()

            y_step(s)

            @pl.when(s == 0)
            def _():
                in_weights().wait()

            h_step(s)

        @pl.when(s == nc)
        def _():
            operands(dy, acat)
            odd_steps(True, 0, na)

        @pl.when(s == nc + 1)
        def _():
            even_steps(True, 0, na)

        @pl.when((s == nc + 2) | (s == nc + 3))
        def _():
            @pl.when(s == nc + 2)
            def _():
                operands(h, dcat)

            second = s - (nc + 2)
            odd_steps(False, second * half_b, jnp.where(second == 0, half_b, nb))

        @pl.when((s == nc + 4) | (s == nc + 5))
        def _():
            second = s - (nc + 4)
            even_steps(False, second * half_b, jnp.where(second == 0, half_b, nb))

        return carry

    lax.fori_loop(0, 2 * nc + 6, step, 0)
    far_waits(True)
    far_waits(False)
    store = local(gv, gsum, load.at[0])
    store.start()
    store.wait()


def back_call(acat, wod, gate, up, dact, dq, wcat, h, dy, x, dhkv, gain, nc=6, col=512, tile=512):
    tok, width = h.shape
    ka, kb = acat.shape[1], wcat.shape[1]
    ff = gate.shape[1]
    cr = tok // (2 * nc)
    rt_rows = 2 * cr
    blk, mid = width // 8, width // 2
    na, nb = ka // tile, kb // tile
    big = max(mid, 2 * tile)
    shape = jax.ShapeDtypeStruct
    outs = (
        shape((2, tok, width), BF16), shape((2, tok, width), BF16), shape((2, 2 * nc, cr, width), BF16), shape((tok, kb), BF16),
        shape((ka, mid), F32), shape((mid, kb), F32), shape((ka, blk), F32), shape((blk, kb), F32),
        shape((3, ka, blk), WIRE), shape((3, blk, kb), WIRE), shape((16, width), F32),
    )
    scratch = [
        pltpu.VMEM((max(ka, tok), width), BF16), pltpu.VMEM((max(width, tok), max(ka, kb)), BF16),
        pltpu.VMEM((rt_rows, max(ka, kb)), BF16), pltpu.VMEM((rt_rows, width), BF16),
        pltpu.VMEM((rt_rows, ff), BF16), pltpu.VMEM((rt_rows, ff), BF16), pltpu.VMEM((rt_rows, ff), BF16),
        pltpu.VMEM((big, big), F32), pltpu.VMEM((big, big), F32),
        pltpu.VMEM((2, 3, tile, blk), WIRE), pltpu.VMEM((2, 3, blk, tile), WIRE),
        pltpu.VMEM((cr, width), BF16), pltpu.VMEM((cr, width), BF16), pltpu.VMEM((2, 2, cr, width), BF16),
        pltpu.VMEM((cr, width), BF16), pltpu.VMEM((cr, width), BF16), pltpu.VMEM((cr, width), F32),
        pltpu.VMEM((16, width), F32),
        pltpu.SemaphoreType.DMA((5,)), pltpu.SemaphoreType.DMA((9,)), pltpu.SemaphoreType.DMA,
        pltpu.SemaphoreType.DMA((5,)), pltpu.SemaphoreType.DMA((2, 2)),
        pltpu.SemaphoreType.DMA((2, 2 * nc)), pltpu.SemaphoreType.DMA((2, 2 * nc)),
        pltpu.SemaphoreType.DMA((2, 2 * nc)), pltpu.SemaphoreType.DMA((2, 2 * nc)),
        pltpu.SemaphoreType.DMA((na + nb,)), pltpu.SemaphoreType.DMA((na + nb,)),
        pltpu.SemaphoreType.DMA((3, na + nb)), pltpu.SemaphoreType.DMA((3, na + nb)),
        pltpu.SemaphoreType.DMA((3,)),
    ]
    flops = 2 * tok * width * (2 * ka + 2 * kb)
    anywhere = pl.BlockSpec(memory_space=pl.ANY)
    return pl.pallas_call(
        functools.partial(back_kernel, (nc, cr, col, tile)),
        out_shape=outs,
        in_specs=[anywhere] * 12,
        out_specs=tuple(anywhere for _ in outs),
        scratch_shapes=scratch,
        cost_estimate=pl.CostEstimate(flops=2 * flops, bytes_accessed=200_000_000, transcendentals=tok * ff),
        compiler_params=pltpu.CompilerParams(vmem_limit_bytes=67_000_000, has_side_effects=True),
        name='backward',
    )(acat, wod, gate, up, dact, dq, wcat, h, dy, x, dhkv, gain)


def solution(mesh):
    def device_step(x_in, dy_out, ln_gain, w_q, w_k, w_v, w_o, w_gate, w_up, w_down):
        n_batch, seq_len, width = x_in.shape
        head_dim = w_k.shape[1]
        inner = w_q.shape[1]
        ff = w_gate.shape[1]
        tok = n_batch * seq_len
        nc = 6
        cr = tok // (2 * nc)
        z = lax.axis_index('tp')
        far = z >= 2
        owner = (z == 0) | (z == 3)

        wqkv = gather(jnp.concatenate([w_q, w_k, w_v], axis=1), 0)
        wkv = wqkv[:, inner:]

        gain = lax.all_gather(ln_gain, 'fsdp', tiled=True)
        x_rows = x_in.reshape(tok, width)
        dy = dy_out.reshape(tok, width)
        h_norm = layer_norm(x_rows.astype(F32), gain)

        wod = gather(after(jnp.concatenate([w_o, w_down], axis=0), h_norm), 1)
        wo = wod[:inner]
        wd = wod[inner:]
        qkv = mm('sd,de->se', h_norm, wqkv).astype(BF16).reshape(n_batch, seq_len, -1)
        wg = gather(after(w_gate, qkv), 0)
        cos_t, sin_t = rope_tables(seq_len, head_dim)
        q_raw = qkv[..., :inner].reshape(n_batch, seq_len, -1, head_dim)
        k_raw = qkv[..., inner:inner + head_dim]
        v_val = qkv[..., inner + head_dim:]

        def q_post(q):
            return (rotate(q.astype(F32), cos_t[:, None, :], sin_t[:, None, :]) * (1.0 / math.sqrt(head_dim))).astype(BF16)

        q_rot, q_pull = jax.vjp(q_post, q_raw)
        k_rot = rotate(k_raw.astype(F32), cos_t, sin_t).astype(BF16)
        att_out, att_pull = jax.vjp(attend, q_rot, k_rot, v_val)
        att = att_out.reshape(tok, inner)
        wu = gather(after(w_up, att), 0)

        d_att = mm('sd,ed->se', dy, wo).astype(BF16).reshape(n_batch, seq_len, -1, head_dim)
        d_act = mm('sd,fd->sf', dy, wd).astype(BF16)
        d_qrot, dk_part, dv_part = att_pull(d_att)
        (d_qraw,) = q_pull(d_qrot)
        d_q = d_qraw.reshape(tok, inner)

        def split(val):
            return val.reshape(nc, 2, cr, -1)

        def own_rows(val):
            parts = split(val)
            return jnp.where(far, parts[:, 0], parts[:, 1]).reshape(nc * cr, -1)

        dkv_part = split(jnp.concatenate([dk_part, dv_part], axis=-1))
        kv_r = line_sum(dkv_part[:, 0], z, 1)
        kv_l = line_sum(dkv_part[:, 1], z, -1)
        kv_sum = (jnp.where(far, dkv_part[:, 0], dkv_part[:, 1]).astype(F32) + jnp.where(far, kv_r, kv_l).astype(F32)).reshape(nc * cr, -1)
        d_krot = kv_sum[:, :head_dim].astype(BF16)
        d_val = kv_sum[:, head_dim:].astype(BF16)
        tables = own_rows(jnp.tile(jnp.concatenate([cos_t, sin_t], axis=-1), (n_batch, 1)))
        half_dim = head_dim // 2
        d_kraw = rotate(d_krot.astype(F32), tables[:, :half_dim], -tables[:, half_dim:]).astype(BF16)
        d_kv = jnp.concatenate([d_kraw, d_val], axis=-1)
        dhkv = mm('se,de->sd', d_kv, wkv)
        d_kv_w = jnp.where(owner, d_kv, jnp.zeros_like(d_kv))
        grad_kv = scatter(after(mm('sd,se->de', own_rows(h_norm), d_kv_w), wu), 0)

        gate = mm('sd,df->sf', h_norm, wg).astype(BF16)
        up = mm('sd,df->sf', h_norm, wu).astype(BF16)
        act = swiglu(gate, up)
        acat = jnp.concatenate([att, act], axis=-1)
        wcat = jnp.concatenate([wg, wu, wqkv[:, :inner]], axis=-1)
        gain8 = jnp.concatenate([gain[None, :], jnp.zeros((7, width), F32)], axis=0)

        res = back_call(acat, wod, gate, up, d_act, d_q, wcat, h_norm, dy, x_rows, dhkv, gain8)
        out, own_a, own_b, got_a, got_b, gsum = res[1], res[6], res[7], res[8], res[9], res[10]
        y_out = out[0].reshape(n_batch, seq_len, width)
        grad_x = out[1].reshape(n_batch, seq_len, width)

        def total(own, got):
            return own + got[0].astype(F32) + got[1].astype(F32) + got[2].astype(F32)

        grad_od = total(own_a, got_a)
        grad_in = total(own_b, got_b)
        gain_part = jnp.where(owner, gsum[8], 0.0)
        grad_gain = lax.psum_scatter(lax.psum(gain_part, 'tp'), 'fsdp', scatter_dimension=0, tiled=True)
        grad_kv = lax.psum(grad_kv, 'tp')
        return (y_out, grad_x, grad_gain, grad_in[:, 2 * ff:], grad_kv[:, :head_dim], grad_kv[:, head_dim:], grad_od[:inner],
                grad_in[:, :ff], grad_in[:, ff:2 * ff], grad_od[inner:])

    act_spec = P('fsdp', None, None)
    row_spec = P('fsdp', 'tp')
    kv_spec = P('fsdp', None)
    col_spec = P('tp', 'fsdp')
    in_specs = (act_spec, act_spec, P('fsdp'), row_spec, kv_spec, kv_spec, col_spec, row_spec, row_spec, col_spec)
    out_specs = (act_spec, act_spec, P('fsdp'), row_spec, kv_spec, kv_spec, col_spec, row_spec, row_spec, col_spec)
    return jax.shard_map(device_step, mesh=mesh, in_specs=in_specs, out_specs=out_specs, check_vma=False)
```

```python
import functools
import math
import jax
import jax.numpy as jnp
from jax import lax
from jax.experimental import pallas as pl
from jax.experimental.pallas import tpu as pltpu
from jax.sharding import PartitionSpec as P

F32 = jnp.float32
BF16 = jnp.bfloat16
WIRE = jnp.bfloat16
STEP = 32
ZERO, ONE, TWO, THREE = range(4)


def rope_tables(seq_len, head_dim):
    half_dim = head_dim // 2
    inv_freq = jnp.power(10000.0, -2.0 * jnp.arange(half_dim, dtype=F32) / head_dim)
    angle = jnp.arange(seq_len, dtype=F32)[:, None] * inv_freq[None, :]
    return jnp.cos(angle), jnp.sin(angle)


def row_loop(rows, fn):
    def body(i, carry):
        fn(pl.ds(pl.multiple_of(i * STEP, STEP), STEP))
        return carry

    lax.fori_loop(0, rows // STEP, body, 0)


def contract(left, right, dims):
    return lax.dot_general(left, right, ((dims[:1], dims[1:]), ((), ())), preferred_element_type=F32)


def front_kernel(dims, x, dy, gain, sq, skv, sg, su, sod,
                 wcat, wkv, wod, gain_all, h, qkv, gate, up, act, datt, dact,
                 hv, wv, wodv, wqv, xt, yt, gt, et, b_q, b_kv, b_g, b_od, b_u, gv,
                 load, wload, keep, bsem, gsem, gain_s, gain_r, send, recv):
    rt_rows, col = dims
    tok, width = x.shape
    inner, kv, ff = sq.shape[ONE], skv.shape[ONE], sg.shape[ONE]
    blk = sq.shape[ZERO]
    ka = inner + ff
    n = tok // rt_rows
    me = lax.axis_index('fsdp')

    def local(src, dst, sem):
        return pltpu.make_async_copy(src, dst, sem)

    def remote(src, dst, s, r, to):
        return pltpu.make_async_remote_copy(src_ref=src, dst_ref=dst, send_sem=s, recv_sem=r, device_id={'fsdp': me ^ to},
                                            device_id_type=pl.DeviceIdType.MESH)

    items = (
        (sq, wcat, TWO * ff, inner), (skv, wkv, ZERO, kv), (sg, wcat, ZERO, ff), (sod, wod, ZERO, blk), (su, wcat, ff, ff),
    )

    def block(i, mask, part=None):
        _, full, at, wide = items[i]
        at_blk = pl.multiple_of((me ^ mask) * blk, blk)
        if i == THREE:
            rows = pl.ds(ZERO, ka) if part is None else pl.ds(part * (ka // TWO), ka // TWO)
            return full.at[rows, pl.ds(at_blk, blk)]
        rows = pl.ds(at_blk, blk) if part is None else pl.ds(at_blk + part * (blk // TWO), blk // TWO)
        return full.at[rows, pl.ds(at, wide)]

    def own_to(i, to, num):
        return remote(items[i][ZERO], block(i, ZERO), send.at[i, num], recv.at[i, num], to)

    def pass_to(i, mask, to, num, part=None):
        return remote(block(i, mask, part), block(i, mask, part), send.at[i, num], recv.at[i, num], to)

    def arrived(i, mask, to, num, part=None):
        remote(block(i, mask, part), block(i, mask, part), send.at[i, num], recv.at[i, num], to).wait_recv()

    def depart(i):
        own_to(i, TWO, ZERO).start()
        own_to(i, 4, ONE).start()
        own_to(i, ONE, 4).start()

    def relay(i):
        arrived(i, TWO, TWO, ZERO)
        pass_to(i, TWO, 4, TWO, ZERO).start()
        arrived(i, 4, 4, ONE)
        pass_to(i, 4, TWO, THREE, ONE).start()
        pass_to(i, TWO, ONE, 5).start()
        pass_to(i, 4, ONE, 6).start()

    def corner(i):
        arrived(i, 6, 4, TWO, ZERO)
        pass_to(i, 6, ONE, 7, ZERO).start()
        arrived(i, 6, TWO, THREE, ONE)
        pass_to(i, 6, ONE, 8, ONE).start()

    def full(i):
        arrived(i, ONE, ONE, 4)
        arrived(i, THREE, ONE, 5)
        arrived(i, 5, ONE, 6)
        arrived(i, 7, ONE, 7, ZERO)
        arrived(i, 7, ONE, 8, ONE)

    def sent(i):
        own_to(i, TWO, ZERO).wait_send()
        own_to(i, 4, ONE).wait_send()
        own_to(i, ONE, 4).wait_send()
        pass_to(i, TWO, 4, TWO, ZERO).wait_send()
        pass_to(i, 4, TWO, THREE, ONE).wait_send()
        pass_to(i, TWO, ONE, 5).wait_send()
        pass_to(i, 4, ONE, 6).wait_send()
        pass_to(i, 6, ONE, 7, ZERO).wait_send()
        pass_to(i, 6, ONE, 8, ONE).wait_send()

    bounce = (b_q, b_kv, b_g, b_od, b_u)

    def own_in(i):
        return local(items[i][ZERO], bounce[i], bsem.at[i])

    def own_out(i):
        return local(bounce[i], block(i, ZERO), bsem.at[i])

    def tile_rows(k):
        return pl.ds(pl.multiple_of(k * rt_rows, rt_rows), rt_rows)

    def tiles(fn):
        def body(k, carry):
            fn(k)
            return carry

        lax.fori_loop(ZERO, n, body, ZERO)

    def dot_cols(left, weight, dims_, out, wide, at=ZERO):
        def body(j, carry):
            cs = pl.ds(pl.multiple_of(j * col, col), col)
            rhs = weight[:, cs] if dims_[ONE] == ZERO else weight[cs, :]
            out[:, pl.ds(pl.multiple_of(at + j * col, col), col)] = contract(left[...], rhs, dims_).astype(BF16)
            return carry

        lax.fori_loop(ZERO, wide // col, body, ZERO)

    def gain_cols(mask):
        return pl.ds(pl.multiple_of((me ^ mask) * blk, blk), blk)

    def gain_to(m):
        return remote(gain, gain_all.at[:, gain_cols(ZERO)], gain_s.at[m - ONE], gain_r.at[m - ONE], m)

    def gain_from(m):
        return remote(gain, gain_all.at[:, gain_cols(m)], gain_s.at[m - ONE], gain_r.at[m - ONE], m)

    def gain_in(m):
        return local(gain if m == ZERO else gain_all.at[:, gain_cols(m)], gv.at[:, gain_cols(m)], gsem.at[m])

    peers = range(ONE, 8)
    for m in peers:
        gain_to(m).start()
    for i in range(THREE):
        depart(i)
    gain_in(ZERO).start()
    for i in range(5):
        own_in(i).start()
    for m in peers:
        gain_from(m).wait_recv()
        gain_in(m).start()
    for i in range(5):
        own_in(i).wait()
        own_out(i).start()
    for m in range(8):
        gain_in(m).wait()

    def x_load(k):
        return local(x.at[tile_rows(k)], xt.at[lax.rem(k, TWO)], load.at[lax.rem(k, TWO)])

    def h_keep(k):
        return local(hv.at[tile_rows(k)], h.at[tile_rows(k)], keep.at[lax.rem(k, TWO)])

    x_load(ZERO).start()

    def norm(k):
        x_load(k).wait()

        @pl.when(k + ONE < n)
        def _():
            x_load(k + ONE).start()

        def rows(sl):
            xv = xt[lax.rem(k, TWO), sl, :].astype(F32)
            cent = xv - jnp.mean(xv, axis=-ONE, keepdims=True)
            inv = lax.rsqrt(jnp.mean(cent * cent, axis=-ONE, keepdims=True) + 1e-5)
            hv[pl.ds(pl.multiple_of(k * rt_rows + sl.start, STEP), STEP), :] = (cent * inv * gv[ZERO:ONE, :]).astype(BF16)

        row_loop(rt_rows, rows)

        @pl.when(k >= TWO)
        def _():
            h_keep(k - TWO).wait()

        h_keep(k).start()

    tiles(norm)
    h_keep(n - TWO).wait()
    h_keep(n - ONE).wait()

    for i in range(THREE):
        relay(i)
    depart(THREE)
    for i in range(TWO):
        corner(i)
    for i in range(5):
        own_out(i).wait()
    for i in range(TWO):
        full(i)
    w0 = local(wcat.at[:, pl.ds(TWO * ff, inner)], wqv.at[:, pl.ds(ZERO, inner)], wload.at[ZERO])
    w1 = local(wkv, wqv.at[:, pl.ds(inner, kv)], wload.at[ONE])
    w0.start()
    w1.start()
    w0.wait()
    w1.wait()

    def out_keep(k, src, dst, which):
        return local(src, dst.at[tile_rows(k)], keep.at[which])

    def qkv_tile(k):
        @pl.when(k >= ONE)
        def _():
            out_keep(k - ONE, yt.at[:, pl.ds(ZERO, inner + kv)], qkv, TWO).wait()

        dot_cols(hv.at[tile_rows(k)], wqv, (ONE, ZERO), yt, inner + kv)
        out_keep(k, yt.at[:, pl.ds(ZERO, inner + kv)], qkv, TWO).start()

    tiles(qkv_tile)
    out_keep(n - ONE, yt.at[:, pl.ds(ZERO, inner + kv)], qkv, TWO).wait()

    corner(TWO)
    full(TWO)
    w2 = local(wcat.at[:, pl.ds(ZERO, ff)], wv, wload.at[TWO])
    w2.start()
    w2.wait()

    def gate_tile(k):
        @pl.when(k >= ONE)
        def _():
            out_keep(k - ONE, yt.at[:, pl.ds(ZERO, ff)], gate, TWO).wait()

        dot_cols(hv.at[tile_rows(k)], wv, (ONE, ZERO), yt, ff)
        out_keep(k, yt.at[:, pl.ds(ZERO, ff)], gate, TWO).start()

    tiles(gate_tile)
    out_keep(n - ONE, yt.at[:, pl.ds(ZERO, ff)], gate, TWO).wait()

    def dy_load(k):
        return local(dy.at[tile_rows(k)], xt.at[lax.rem(k, TWO)], load.at[lax.rem(k, TWO)])

    dy_load(ZERO).start()
    relay(THREE)
    depart(4)
    corner(THREE)
    full(THREE)
    w3 = local(wod, wodv, wload.at[THREE])
    w3.start()
    w3.wait()

    def back_keeps(k):
        return (local(yt.at[:, pl.ds(ZERO, inner)], datt.at[tile_rows(k)], keep.at[TWO]),
                local(yt.at[:, pl.ds(inner, ff)], dact.at[tile_rows(k)], keep.at[THREE]))

    def back_tile(k):
        dy_load(k).wait()

        @pl.when(k + ONE < n)
        def _():
            dy_load(k + ONE).start()

        @pl.when(k == (TWO * n) // THREE)
        def _():
            relay(4)

        @pl.when(k >= ONE)
        def _():
            for c in back_keeps(k - ONE):
                c.wait()

        dot_cols(xt.at[lax.rem(k, TWO)], wodv, (ONE, ONE), yt, ka)
        for c in back_keeps(k):
            c.start()

    tiles(back_tile)
    for c in back_keeps(n - ONE):
        c.wait()

    def gate_load(k):
        return local(gate.at[tile_rows(k)], gt, load.at[TWO])

    gate_load(ZERO).start()
    corner(4)
    full(4)
    w4 = local(wcat.at[:, pl.ds(ff, ff)], wv, wload.at[4])
    w4.start()
    w4.wait()

    def up_keeps(k):
        return (local(yt.at[:, pl.ds(ZERO, ff)], up.at[tile_rows(k)], keep.at[TWO]), local(et, act.at[tile_rows(k)], keep.at[THREE]))

    def up_tile(k):
        @pl.when(k >= ONE)
        def _():
            for c in up_keeps(k - ONE):
                c.wait()

        dot_cols(hv.at[tile_rows(k)], wv, (ONE, ZERO), yt, ff)
        gate_load(k).wait()

        def rows(sl):
            g = gt[sl, :].astype(F32)
            et[sl, :] = (g * jax.nn.sigmoid(g) * yt[sl, ZERO:ff].astype(F32)).astype(BF16)

        row_loop(rt_rows, rows)

        @pl.when(k + ONE < n)
        def _():
            gate_load(k + ONE).start()

        for c in up_keeps(k):
            c.start()

    tiles(up_tile)
    for c in up_keeps(n - ONE):
        c.wait()
    for i in range(5):
        sent(i)
    for m in peers:
        gain_to(m).wait_send()
    g_out = local(gv.at[:, gain_cols(ZERO)], gain_all.at[:, gain_cols(ZERO)], gsem.at[ZERO])
    g_out.start()
    g_out.wait()


def front_call(x, dy, gain, sq, skv, sg, su, sod, rt_rows=384, col=512):
    tok, width = x.shape
    inner, kv, ff = sq.shape[1], skv.shape[1], sg.shape[1]
    blk = sq.shape[0]
    ka = inner + ff
    shape = jax.ShapeDtypeStruct
    outs = (
        shape((width, 2 * ff + inner), BF16), shape((width, kv), BF16), shape((ka, width), BF16), shape((8, width), F32),
        shape((tok, width), BF16), shape((tok, inner + kv), BF16), shape((tok, ff), BF16), shape((tok, ff), BF16), shape((tok, ff), BF16),
        shape((tok, inner), BF16), shape((tok, ff), BF16),
    )
    sems = pltpu.SemaphoreType.DMA
    scratch = [
        pltpu.VMEM((tok, width), BF16), pltpu.VMEM((width, ff), BF16), pltpu.VMEM((ka, width), BF16), pltpu.VMEM((width, inner + kv), BF16),
        pltpu.VMEM((2, rt_rows, width), BF16), pltpu.VMEM((rt_rows, max(ka, inner + kv)), BF16), pltpu.VMEM((rt_rows, ff), BF16),
        pltpu.VMEM((rt_rows, ff), BF16), pltpu.VMEM(sq.shape, BF16), pltpu.VMEM(skv.shape, BF16), pltpu.VMEM(sg.shape, BF16), pltpu.VMEM(sod.shape, BF16), pltpu.VMEM(su.shape, BF16),
        pltpu.VMEM((8, width), F32),
        sems((3,)), sems((5,)), sems((4,)), sems((5,)), sems((8,)), sems((7,)), sems((7,)), sems((5, 9)), sems((5, 9)),
    ]
    flops = 2 * tok * width * (2 * ka + ff + kv)
    anywhere = pl.BlockSpec(memory_space=pl.ANY)
    return pl.pallas_call(
        functools.partial(front_kernel, (rt_rows, col)),
        out_shape=outs,
        in_specs=[anywhere] * 8,
        out_specs=tuple(anywhere for _ in outs),
        scratch_shapes=scratch,
        cost_estimate=pl.CostEstimate(flops=flops, bytes_accessed=150_000_000, transcendentals=tok * ff),
        compiler_params=pltpu.CompilerParams(vmem_limit_bytes=67_000_000, has_side_effects=True),
        name='forward',
    )(x, dy, gain, sq, skv, sg, su, sod)


def back_kernel(dims, att, act, wod, gate, up, dact, dq, wcat, wkv, dkv, table, h, dy, x, gain,
                y_out, gx_out, part, line, kvline, dcat, dhkv, peer_a, peer_b, own_a, own_b, got_a, got_b, gsum, gtmp, kvsum, snd_a, snd_b,
                wa, wb, st, wv, tv, ctile, gt, ot, rt, sa, sb, zr, zo, zs, zx, zd, zk, kr, ko, kz, gv, kw, gw,
                load, wload, wait_y, zload, zstore, kstore, rs_s, rs_r, kv_s, kv_r, ag_s, ag_r, core_s, core_r, far_s, far_r, own_s, put_s, kf_s, kf_r, kf_l, gl_s, gf_s, gf_r, gz_s, gz_r):
    nc, cr, col, tile = dims
    tok, width = h.shape
    inner, ff = att.shape[ONE], act.shape[ONE]
    ka, kb = inner + ff, wcat.shape[ONE]
    kv = dkv.shape[ONE]
    head = kv // TWO
    n_pos = table.shape[ZERO]
    rt_rows = 4 * cr
    blk = width // 8
    mid = width // TWO
    na, nb = ka // tile, (kb + kv) // tile
    depth = THREE
    last = THREE
    hop_lag = TWO
    end = TWO * nc - ONE + hop_lag * (last + TWO)
    me = lax.axis_index('fsdp')
    z = lax.axis_index('tp')

    def remote(src, dst, send, recv, **to):
        return pltpu.make_async_remote_copy(src_ref=src, dst_ref=dst, send_sem=send, recv_sem=recv,
                                            device_id=to, device_id_type=pl.DeviceIdType.MESH)

    def local(src, dst, sem):
        return pltpu.make_async_copy(src, dst, sem)

    def chunk_row(d, c):
        return pl.multiple_of(lax.rem(c, nc) * (TWO * cr) + d * cr, cr)

    def chunk_rows(d, c):
        return pl.ds(chunk_row(d, c), cr)

    def slot_parts(t):
        parts = []
        up_z, down_z = lax.rem(z + ONE, last + ONE), lax.rem(z + last, last + ONE)
        for d in range(TWO):
            parts.append(line_parts(t, d, up_z, down_z))
        return parts

    def line_parts(t, d, up_z, down_z):
        if True:
            rank = z if d == ZERO else last - z
            fwd, back = (up_z, down_z) if d == ZERO else (down_z, up_z)

            def hop(c, src=None):
                src = part.at[lax.div(c, nc), chunk_rows(d, c)] if src is None else src
                return remote(src, line.at[d, c], rs_s.at[d, c], rs_r.at[d, c], tp=fwd)

            def mid_hop(c):
                return hop(c, zs.at[d, lax.rem(c, depth)])

            def kv_hop(c, src=None):
                src = dkv.at[chunk_rows(d, c)] if src is None else src
                return remote(src, kvline.at[d, c], kv_s.at[d, c], kv_r.at[d, c], tp=fwd)

            def mid_kv_hop(c):
                return kv_hop(c, kz.at[d, lax.rem(c, depth)])

            def bcast_of(c, dst, src=None):
                src = dst.at[chunk_rows(d, c)] if src is None else src
                return remote(src, dst.at[chunk_rows(d, c)], ag_s.at[d, c], ag_r.at[d, c], tp=back)

            def keep_of(c, dst):
                return local(zs.at[d, lax.rem(c, depth)], dst.at[chunk_rows(d, c)], zstore.at[d, lax.rem(c, depth)])

            def for_kind(c, fn):
                @pl.when(c < nc)
                def _():
                    fn(y_out)

                @pl.when(c >= nc)
                def _():
                    fn(gx_out)

            def depart():
                @pl.when((rank == ZERO) & (t >= ZERO) & (t < TWO * nc))
                def _():
                    hop(t).start()

                    @pl.when(t < nc)
                    def _():
                        kv_hop(t).start()

            c = t - hop_lag * rank
            rows = chunk_rows(d, c)
            own = pl.ds(pl.multiple_of(lax.rem(c, nc) * cr, cr), cr)

            def load_of(i):
                return (
                    local(part.at[lax.div(c, nc), rows], zo.at[d], zload.at[d, ZERO]), local(line.at[d, c], zr.at[d], zload.at[d, ONE]),
                    local(x.at[rows], zx, zload.at[d, TWO]), local(dy.at[rows], zd, zload.at[d, THREE]),
                    local(dhkv.at[own], zk, zload.at[d, 4]), local(dkv.at[rows], ko.at[d], zload.at[d, 5]),
                    local(kvline.at[d, lax.rem(c, nc)], kr.at[d], zload.at[d, 6]),
                )[i]

            busy = (rank > ZERO) & (c >= ZERO) & (c < TWO * nc)

            def begin():
                @pl.when(busy)
                def _():
                    load_of(ZERO).start()

                    @pl.when(rank == last)
                    def _():
                        load_of(TWO).start()

                        @pl.when(c >= nc)
                        def _():
                            load_of(THREE).start()

                    hop(c).wait_recv()
                    load_of(ONE).start()

                    @pl.when(c < nc)
                    def _():
                        load_of(5).start()
                        kv_hop(c).wait_recv()
                        load_of(6).start()

            def finish():
                @pl.when(busy & (rank < last))
                def _():
                    @pl.when(c >= depth)
                    def _():
                        mid_hop(c - depth).wait_send()

                    load_of(ZERO).wait()
                    load_of(ONE).wait()

                    def add(sl):
                        zs[d, lax.rem(c, depth), sl, :] = (zr[d, sl, :].astype(F32) + zo[d, sl, :].astype(F32)).astype(BF16)

                    row_loop(cr, add)
                    mid_hop(c).start()

                    @pl.when(c < nc)
                    def _():
                        @pl.when(c >= depth)
                        def _():
                            mid_kv_hop(c - depth).wait_send()

                        load_of(5).wait()
                        load_of(6).wait()
                        kz[d, lax.rem(c, depth)] = (kr[d].astype(F32) + ko[d].astype(F32)).astype(BF16)
                        mid_kv_hop(c).start()

                @pl.when(busy & (rank == last))
                def _():
                    @pl.when(c >= nc)
                    def _():
                        load_of(4).start()

                    @pl.when(c >= depth)
                    def _():
                        bcast_of(c - depth, y_out).wait_send()
                        keep_of(c - depth, y_out).wait()

                    load_of(ZERO).wait()
                    load_of(ONE).wait()
                    load_of(TWO).wait()

                    @pl.when(c < nc)
                    def _():
                        def fin(sl):
                            branch = zr[d, sl, :].astype(F32) + zo[d, sl, :].astype(F32)
                            zs[d, lax.rem(c, depth), sl, :] = (zx[sl, :].astype(F32) + branch).astype(BF16)

                        row_loop(cr, fin)

                    @pl.when(c >= nc)
                    def _():
                        load_of(THREE).wait()
                        load_of(4).wait()

                        def fin(sl):
                            dh = (zr[d, sl, :].astype(F32) + zo[d, sl, :].astype(F32) + zk[sl, :]).astype(BF16).astype(F32)
                            xv = zx[sl, :].astype(F32)
                            cent = xv - jnp.mean(xv, axis=-ONE, keepdims=True)
                            inv = lax.rsqrt(jnp.mean(cent * cent, axis=-ONE, keepdims=True) + 1e-5)
                            hat = cent * inv
                            gv[8:9, :] = gv[8:9, :] + jnp.sum(dh * hat, axis=ZERO, keepdims=True)
                            dn = dh * gv[ZERO:ONE, :]
                            dx = inv * (dn - jnp.mean(dn, axis=-ONE, keepdims=True)
                                        - hat * jnp.mean(dn * hat, axis=-ONE, keepdims=True))
                            zs[d, lax.rem(c, depth), sl, :] = (zd[sl, :].astype(F32) + dx).astype(BF16)

                        row_loop(cr, fin)

                    for_kind(c, lambda dst: keep_of(c, dst).start())
                    for_kind(c, lambda dst: bcast_of(c, dst, zs.at[d, lax.rem(c, depth)]).start())

                    @pl.when(c < nc)
                    def _():
                        load_of(5).wait()
                        load_of(6).wait()
                        pos = pl.ds(pl.multiple_of(lax.rem(chunk_row(d, c), n_pos), cr), cr)
                        cos_t, sin_t = tv[pos, ZERO:head // TWO], tv[pos, head // TWO:head]

                        def summed(lo, hi):
                            return (kr[d, :, lo:hi].astype(F32) + ko[d, :, lo:hi].astype(F32)).astype(BF16)

                        first = summed(ZERO, head // TWO).astype(F32)
                        second = summed(head // TWO, head).astype(F32)
                        kz[d, ZERO, :, ZERO:head // TWO] = (first * cos_t + second * sin_t).astype(BF16)
                        kz[d, ZERO, :, head // TWO:head] = (second * cos_t - first * sin_t).astype(BF16)
                        kz[d, ZERO, :, head:kv] = summed(head, kv)
                        keep_kv = local(kz.at[d, ZERO], dcat.at[rows, pl.ds(kb, kv)], kstore.at[ZERO])
                        keep_kv.start()

                        def cols(j, carry):
                            cs = pl.ds(pl.multiple_of(j * col, col), col)
                            zk[:, cs] = contract(kz[d, ZERO], wv[cs, :], (ONE, ONE))
                            return carry

                        lax.fori_loop(ZERO, width // col, cols, ZERO)
                        keep_h = local(zk, dhkv.at[own], kstore.at[ONE])
                        keep_h.start()
                        keep_kv.wait()
                        keep_h.wait()

            e = t - hop_lag * (last + ONE) - hop_lag * (TWO - rank)

            def pass_on():
                @pl.when(((rank == ONE) | (rank == TWO)) & (e >= ZERO) & (e < TWO * nc))
                def _():
                    bcast_of(e, y_out).wait_recv()
                    for_kind(e, lambda dst: bcast_of(e, dst).start())

            def settle():
                def each(c, carry):
                    tail = TWO * nc - depth
                    kv_tail = (c >= nc - depth) & (c < nc)

                    @pl.when(rank == ZERO)
                    def _():
                        hop(c).wait_send()
                        bcast_of(c, y_out).wait_recv()

                        @pl.when(c < nc)
                        def _():
                            kv_hop(c).wait_send()

                    @pl.when((rank == ONE) | (rank == TWO))
                    def _():
                        bcast_of(c, y_out).wait_send()

                        @pl.when(c >= tail)
                        def _():
                            mid_hop(c).wait_send()

                        @pl.when(kv_tail)
                        def _():
                            mid_kv_hop(c).wait_send()

                    @pl.when((rank == last) & (c >= tail))
                    def _():
                        bcast_of(c, y_out).wait_send()
                        keep_of(c, y_out).wait()

                    return carry

                lax.fori_loop(ZERO, TWO * nc, each, ZERO)

            return depart, begin, finish, pass_on, settle

    def slot(t):
        parts = slot_parts(t)
        for i in range(4):
            for p in parts:
                p[i]()

        @pl.when(t == end)
        def _():
            for p in parts:
                p[4]()

    def gain_total():
        low = pl.ds(8, 8)
        which = lax.div(z, last)

        def cols(mask):
            return pl.ds(pl.multiple_of((me ^ mask) * blk, blk), blk)

        def plane(m):
            return remote(gv.at[low, cols(m)], gtmp.at[m], gf_s.at[m], gf_r.at[m], fsdp=me ^ m)

        def along(i):
            return remote(gw.at[ZERO], gsum.at[which], gz_s.at[i], gz_r.at[which], tp=lax.rem(z + ONE + i, last + ONE))

        def arrived(w):
            remote(gw.at[ZERO], gsum.at[w], gz_s.at[ZERO], gz_r.at[w], tp=lax.rem(z + ONE, last + ONE)).wait_recv()

        peers = range(ONE, 8)

        @pl.when((z == ZERO) | (z == last))
        def _():
            for m in peers:
                plane(m).start()
            own = local(gv.at[low, cols(ZERO)], gw.at[ZERO], gl_s.at[ZERO])
            own.start()
            for m in peers:
                plane(m).wait_recv()
                local(gtmp.at[m], gw.at[m], gl_s.at[m]).start()
            own.wait()
            for m in peers:
                local(gtmp.at[m], gw.at[m], gl_s.at[m]).wait()
            gw[ZERO] = jnp.sum(gw[...], axis=ZERO)
            home = local(gw.at[ZERO], gsum.at[which], gl_s.at[ZERO])
            home.start()
            for i in range(THREE):
                along(i).start()
            home.wait()
            for m in peers:
                plane(m).wait_send()

        @pl.when(z != ZERO)
        def _():
            arrived(ZERO)

        @pl.when(z != last)
        def _():
            arrived(ONE)

        @pl.when((z == ZERO) | (z == last))
        def _():
            for i in range(THREE):
                along(i).wait_send()

    def tile_rows(k):
        return pl.ds(pl.multiple_of(k * rt_rows, rt_rows), rt_rows)

    def y_step(k):
        srcs = [local(att.at[tile_rows(k)], ctile.at[:, pl.ds(ZERO, inner)], load.at[ZERO]),
                local(act.at[tile_rows(k)], ctile.at[:, pl.ds(inner, ff)], load.at[ONE])]
        for s in srcs:
            s.start()
        for s in srcs:
            s.wait()

        def cols(j, carry):
            cs = pl.ds(pl.multiple_of(j * col, col), col)
            gt[:, cs] = contract(ctile[:, ZERO:ka], wa[ZERO:ka, cs], (ONE, ZERO)).astype(BF16)
            return carry

        lax.fori_loop(ZERO, width // col, cols, ZERO)
        dst = local(gt.at[:, pl.ds(ZERO, width)], part.at[ZERO, tile_rows(k)], wait_y)
        dst.start()
        dst.wait()

    def h_step(k):
        rows = tile_rows(k)
        srcs = [local(gate.at[rows], gt.at[:, pl.ds(ZERO, ff)], load.at[ZERO]), local(up.at[rows], ctile.at[:, pl.ds(ZERO, ff)], load.at[ONE]),
                local(dact.at[rows], ctile.at[:, pl.ds(ff, ff)], load.at[TWO]), local(dq.at[rows], ctile.at[:, pl.ds(TWO * ff, kb - TWO * ff)], load.at[THREE])]
        for s in srcs:
            s.start()
        for s in srcs:
            s.wait()

        def act_back(sl):
            g = gt[sl, ZERO:ff].astype(F32)
            u = ctile[sl, ZERO:ff].astype(F32)
            d_act = ctile[sl, ff:TWO * ff].astype(F32)
            sig = jax.nn.sigmoid(g)
            ctile[sl, ZERO:ff] = (d_act * u * (sig + g * sig * (1.0 - sig))).astype(BF16)
            ctile[sl, ff:TWO * ff] = (d_act * (g * sig)).astype(BF16)

        row_loop(rt_rows, act_back)
        keep = local(ctile, dcat.at[rows, pl.ds(ZERO, kb)], load.at[4])
        keep.start()

        def cols(j, carry):
            cs = pl.ds(pl.multiple_of(j * col, col), col)
            gt[:, cs] = contract(ctile[...], wb[cs, ZERO:kb], (ONE, ONE)).astype(BF16)
            return carry

        lax.fori_loop(ZERO, width // col, cols, ZERO)
        dst = local(gt.at[:, pl.ds(ZERO, width)], part.at[ONE, rows], wait_y)
        dst.start()
        dst.wait()
        keep.wait()

    def out_weights():
        return local(wod, wa.at[pl.ds(ZERO, ka)], wload.at[ZERO])

    def in_weights():
        return local(wcat, wb.at[pl.ds(ZERO, width), pl.ds(ZERO, kb)], wload.at[10])

    def operand(src):
        cps = []
        for q in range(8):
            mask = TWO * (q % 4) + q // 4
            cols = pl.ds(pl.multiple_of((me ^ mask) * blk, blk), blk)
            cps.append(local(src.at[:, cols], wa.at[pl.ds(ZERO, tok), pl.ds(q * blk, blk)], wload.at[q]))
        for c in cps:
            c.start()
        for c in cps:
            c.wait()

    first_b = -(-nb // TWO)

    def strip(is_a, k):
        if is_a:
            return k
        return jnp.where(k < first_b, k, jnp.where(k == first_b, nb - ONE, k - ONE))

    def wide_start(is_a, k):
        dst = st.at[lax.rem(k, TWO)]
        sem = wload.at[8 + lax.rem(k, TWO)]
        if is_a:
            @pl.when(k == ZERO)
            def _():
                local(att, dst, sem).start()

            @pl.when(k > ZERO)
            def _():
                local(act.at[:, pl.ds(pl.multiple_of((k - ONE) * tile, tile), tile)], dst, sem).start()
        else:
            local(dcat.at[:, pl.ds(pl.multiple_of(strip(is_a, k) * tile, tile), tile)], dst, sem).start()

    def wide(is_a, k, hi):
        local(dcat.at[:, pl.ds(ZERO, tile)], st.at[lax.rem(k, TWO)], wload.at[8 + lax.rem(k, TWO)]).wait()

        @pl.when(k + ONE < hi)
        def _():
            wide_start(is_a, k + ONE)

    def prod(is_a, k, odd):
        half = pl.ds(odd * mid, mid)
        if is_a:
            return contract(st[lax.rem(k, TWO)], wa[ZERO:tok, half], (ZERO, ZERO))
        return contract(wa[ZERO:tok, half], st[lax.rem(k, TWO)], (ZERO, ZERO))

    def place(ref, is_a, k):
        par = pl.multiple_of(lax.rem(k, TWO) * tile, tile)
        return ref.at[pl.ds(par, tile), :] if is_a else ref.at[:, pl.ds(par, tile)]

    def whole(ref, is_a, k):
        cs = pl.ds(pl.multiple_of(strip(is_a, k) * tile, tile), tile)
        return ref.at[cs, :] if is_a else ref.at[:, cs]

    def piece(ref, is_a, q):
        return ref.at[:, pl.ds(q * blk, blk)] if is_a else ref.at[pl.ds(q * blk, blk), :]

    def away(is_a, k, q):
        base, snd, got = (ZERO, snd_a, got_a) if is_a else (na, snd_b, got_b)
        return remote(whole(snd.at[q], is_a, k), whole(got.at[q], is_a, k), far_s.at[q, base + k], far_r.at[q, base + k],
                      fsdp=me ^ (TWO * (q + ONE)))

    def odd_steps(is_a, lo, hi, stop):
        base = ZERO if is_a else na
        peer = peer_a if is_a else peer_b

        def send(k):
            return remote(place(ot, is_a, k), whole(peer, is_a, k), core_s.at[base + k], core_r.at[base + k], fsdp=me ^ ONE)

        def one(k, carry):
            wide(is_a, k, hi)

            @pl.when(k >= stop[ZERO] + TWO)
            def _():
                send(k - TWO).wait_send()

            place(ot, is_a, k)[...] = prod(is_a, k, ONE)
            send(k).start()

            @pl.when(k == stop[ONE] - ONE)
            def _():
                send(k - ONE).wait_send()
                send(k).wait_send()

            return carry

        wide_start(is_a, lo)
        lax.fori_loop(lo, hi, one, ZERO)

    def even_steps(is_a, lo, hi, stop):
        base = ZERO if is_a else na
        peer, own, snd = (peer_a, own_a, snd_a) if is_a else (peer_b, own_b, snd_b)
        stage = sa if is_a else sb

        def take(k):
            return remote(place(ot, is_a, k), whole(peer, is_a, k), core_s.at[base + k], core_r.at[base + k], fsdp=me ^ ONE)

        def fetch(k):
            if not is_a:
                return [local(whole(peer, is_a, k), rt, own_s.at[TWO])]
            rows = pl.ds(pl.multiple_of(k * tile, tile), tile)
            return [local(peer.at[rows, pl.ds(i * tile, tile)], rt.at[pl.ds(i * tile, tile)], own_s.at[TWO + i])
                    for i in range(mid // tile)]

        def fetched():
            if not is_a:
                return rt[...]
            return jnp.concatenate([rt[i * tile:(i + ONE) * tile, :] for i in range(mid // tile)], axis=ONE)

        def mine(k):
            return local(piece(place(ot, is_a, k), is_a, ZERO), whole(own, is_a, k), own_s.at[lax.rem(k, TWO)])

        def put(k, q):
            return local(stage.at[lax.rem(k, TWO), q], whole(snd.at[q], is_a, k), put_s.at[lax.rem(k, TWO), q])

        def ship(k):
            for q in range(THREE):
                put(k, q).wait()
                away(is_a, k, q).start()

        def one(k, carry):
            take(k).wait_recv()
            for f in fetch(k):
                f.start()
            wide(is_a, k, hi)

            @pl.when(k >= stop[ZERO] + TWO)
            def _():
                mine(k - TWO).wait()

            acc = prod(is_a, k, ZERO)

            @pl.when(k >= stop[ZERO] + ONE)
            def _():
                ship(k - ONE)

            for f in fetch(k):
                f.wait()
            place(ot, is_a, k)[...] = acc + fetched()
            mine(k).start()
            for q in range(THREE):
                stage[lax.rem(k, TWO), q] = piece(place(ot, is_a, k), is_a, q + ONE)[...].astype(WIRE)
                put(k, q).start()

            @pl.when(k == stop[ONE] - ONE)
            def _():
                ship(k)
                mine(k - ONE).wait()
                mine(k).wait()

            return carry

        wide_start(is_a, lo)
        lax.fori_loop(lo, hi, one, ZERO)

    def far_wait(is_a, k):
        for q in range(THREE):
            away(is_a, k, q).wait_recv()

    def far_waits(is_a, but=-ONE):
        def one(k, carry):
            for q in range(THREE):
                away(is_a, k, q).wait_send()

            @pl.when(k != but)
            def _():
                far_wait(is_a, k)

            return carry

        lax.fori_loop(ZERO, na if is_a else nb, one, ZERO)

    def kv_send(i):
        which = lax.div(z, last)
        return remote(kw, kvsum.at[which], kf_s.at[i], kf_r.at[which], tp=lax.rem(z + ONE + i, last + ONE))

    def kv_total():
        @pl.when((z == ZERO) | (z == last))
        def _():
            k = first_b
            cs = pl.ds((nb - ONE) * tile, tile)
            far_wait(False, k)
            own_cp = local(own_b.at[:, cs], kw, load.at[ZERO])
            cps = [local(got_b.at[q, :, cs], sb.at[ZERO, q], load.at[ONE + q]) for q in range(THREE)]
            own_cp.start()
            for cp in cps:
                cp.start()
            own_cp.wait()
            for cp in cps:
                cp.wait()
            kw[...] = kw[...] + sb[ZERO, ZERO].astype(F32) + sb[ZERO, ONE].astype(F32) + sb[ZERO, TWO].astype(F32)
            home = local(kw, kvsum.at[lax.div(z, last)], kf_l)
            home.start()
            for i in range(THREE):
                kv_send(i).start()
            home.wait()

        @pl.when((z != ZERO) & (z != last))
        def _():
            far_wait(False, first_b)

    def kv_settle():
        def arrived(which):
            remote(kw, kvsum.at[which], kf_s.at[ZERO], kf_r.at[which], tp=lax.rem(z + ONE, last + ONE)).wait_recv()

        @pl.when(z != ZERO)
        def _():
            arrived(ZERO)

        @pl.when(z != last)
        def _():
            arrived(ONE)

        @pl.when((z == ZERO) | (z == last))
        def _():
            for i in range(THREE):
                kv_send(i).wait_send()

    out_weights().start()
    in_weights().start()
    gv[8:16, :] = jnp.zeros((8, width), F32)
    small = [local(gain, gv.at[pl.ds(ZERO, 8)], load.at[ZERO]), local(wkv, wv, load.at[ONE]), local(table, tv, load.at[TWO])]
    for s in small:
        s.start()

    ctile[:, ZERO:kv] = jnp.zeros((rt_rows, kv), BF16)
    blanks = [local(ctile.at[:, pl.ds(ZERO, kv)], dcat.at[pl.ds(i * rt_rows, rt_rows), pl.ds(kb, kv)], wload.at[TWO + i])
              for i in range(nc // TWO)]
    for s in blanks:
        s.start()
    for s in blanks + small:
        s.wait()

    steps = nc // TWO
    a_at, h_at, b_at = steps, steps + 4, TWO * steps + 4
    kv_at = b_at + 10
    per_a, per_b = -(-na // TWO), -(-first_b // TWO)

    def share(at, lo, hi, per, i):
        return jnp.minimum(lo + i * per, hi), jnp.minimum(lo + (i + ONE) * per, hi)

    def phase(s, at, n):
        return pl.when((s >= at) & (s < at + n))

    def step(s, carry):
        slot(s - ONE)

        @phase(s, ZERO, steps)
        def _():
            @pl.when(s == ZERO)
            def _():
                out_weights().wait()

            y_step(s)

        @phase(s, a_at, TWO)
        def _():
            @pl.when(s == a_at)
            def _():
                operand(dy)

            odd_steps(True, *share(s, ZERO, na, per_a, s - a_at), (ZERO, na))

        @phase(s, a_at + TWO, TWO)
        def _():
            even_steps(True, *share(s, ZERO, na, per_a, s - (a_at + TWO)), (ZERO, na))

        @phase(s, h_at, steps)
        def _():
            @pl.when(s == h_at)
            def _():
                in_weights().wait()

            h_step(s - h_at)

        for part_b in range(TWO):
            lo, hi = (ZERO, first_b) if part_b == ZERO else (first_b, nb)
            at = b_at + 4 * part_b

            @phase(s, at, TWO)
            def _():
                if part_b == ZERO:
                    @pl.when(s == at)
                    def _():
                        operand(h)

                odd_steps(False, *share(s, lo, hi, per_b, s - at), (lo, hi))

            @phase(s, at + TWO, TWO)
            def _():
                even_steps(False, *share(s, lo, hi, per_b, s - (at + TWO)), (lo, hi))

        @pl.when(s == kv_at)
        def _():
            kv_total()

        @pl.when(s == end - hop_lag * TWO + ONE)
        def _():
            gain_total()

        return carry

    lax.fori_loop(ZERO, end + TWO, step, ZERO)
    far_waits(True)
    far_waits(False, first_b)
    kv_settle()


def back_call(att, act, wod, gate, up, dact, dq, wcat, wkv, dkv, table, h, dy, x, gain, nc=12, col=512, tile=512):
    tok, width = h.shape
    inner, ff = att.shape[1], act.shape[1]
    ka, kb, kv = inner + ff, wcat.shape[1], dkv.shape[1]
    cr = tok // (2 * nc)
    rt_rows = 4 * cr
    blk, mid = width // 8, width // 2
    na, nb = ka // tile, (kb + kv) // tile
    big = max(mid, 2 * tile)
    shape = jax.ShapeDtypeStruct
    outs = (
        shape((tok, width), BF16), shape((tok, width), BF16), shape((2, tok, width), BF16), shape((2, 2 * nc, cr, width), BF16),
        shape((2, nc, cr, kv), BF16), shape((tok, kb + kv), BF16), shape((nc * cr, width), F32),
        shape((ka, mid), F32), shape((mid, kb + kv), F32), shape((ka, blk), F32), shape((blk, kb + kv), F32),
        shape((3, ka, blk), WIRE), shape((3, blk, kb + kv), WIRE), shape((2, 8, blk), F32), shape((8, 8, blk), F32), shape((2, blk, kv), F32),
        shape((3, ka, blk), WIRE), shape((3, blk, kb + kv), WIRE),
    )
    sems = pltpu.SemaphoreType.DMA
    scratch = [
        pltpu.VMEM((max(ka, tok), width), BF16), pltpu.VMEM((width, kb), BF16), pltpu.VMEM((2, tok, tile), BF16),
        pltpu.VMEM((width, kv), BF16), pltpu.VMEM(table.shape, F32),
        pltpu.VMEM((rt_rows, max(ka, kb)), BF16), pltpu.VMEM((rt_rows, max(ff, width)), BF16),
        pltpu.VMEM((big, big), F32), pltpu.VMEM((mid, tile), F32),
        pltpu.VMEM((2, 3, tile, blk), WIRE), pltpu.VMEM((2, 3, blk, tile), WIRE),
        pltpu.VMEM((2, cr, width), BF16), pltpu.VMEM((2, cr, width), BF16), pltpu.VMEM((2, 3, cr, width), BF16),
        pltpu.VMEM((cr, width), BF16), pltpu.VMEM((cr, width), BF16), pltpu.VMEM((cr, width), F32),
        pltpu.VMEM((2, cr, kv), BF16), pltpu.VMEM((2, cr, kv), BF16), pltpu.VMEM((2, 3, cr, kv), BF16),
        pltpu.VMEM((16, width), F32), pltpu.VMEM((blk, kv), F32), pltpu.VMEM((8, 8, blk), F32),
        sems((5,)), sems((11,)), sems, sems((2, 7)), sems((2, 3)), sems((2,)),
        sems((2, 2 * nc)), sems((2, 2 * nc)), sems((2, nc)), sems((2, nc)), sems((2, 2 * nc)), sems((2, 2 * nc)),
        sems((na + nb,)), sems((na + nb,)), sems((3, na + nb)), sems((3, na + nb)), sems((2 + mid // tile,)), sems((2, 3)),
        sems((3,)), sems((2,)), sems, sems((8,)), sems((8,)), sems((8,)), sems((3,)), sems((2,)),
    ]
    flops = 2 * tok * width * (2 * ka + 2 * kb)
    anywhere = pl.BlockSpec(memory_space=pl.ANY)
    return pl.pallas_call(
        functools.partial(back_kernel, (nc, cr, col, tile)),
        out_shape=outs,
        in_specs=[anywhere] * 15,
        out_specs=tuple(anywhere for _ in outs),
        scratch_shapes=scratch,
        cost_estimate=pl.CostEstimate(flops=2 * flops, bytes_accessed=200_000_000, transcendentals=tok * ff),
        compiler_params=pltpu.CompilerParams(vmem_limit_bytes=67_000_000, has_side_effects=True),
        name='backward',
    )(att, act, wod, gate, up, dact, dq, wcat, wkv, dkv, table, h, dy, x, gain)


def attention_kernel(heads, qkv, datt, table, att, dq, dkv, krot, dk_acc, dv_acc):
    n_pos = qkv.shape[0]
    head = qkv.shape[1] // (heads + 2)
    half = head // 2
    scale = 1.0 / math.sqrt(head)
    qb = 256

    def cos_of(sl):
        return table[sl, 0:half], table[sl, half:head]

    def turn(lo, sl, factor):
        cos_t, sin_t = cos_of(sl)
        first = qkv[sl, lo:lo + half].astype(F32)
        second = qkv[sl, lo + half:lo + head].astype(F32)
        return jnp.concatenate([(first * cos_t - second * sin_t) * factor, (second * cos_t + first * sin_t) * factor], axis=-1).astype(BF16)

    k_at, v_at = heads * head, (heads + 1) * head
    krot[...] = turn(k_at, slice(0, n_pos), 1.0)
    dk_acc[...] = jnp.zeros_like(dk_acc)
    dv_acc[...] = jnp.zeros_like(dv_acc)
    for r in range(heads):
        for i in range(n_pos // qb):
            sl = slice(i * qb, (i + 1) * qb)
            upto = (i + 1) * qb
            q = turn(r * head, sl, scale)
            k = krot[0:upto, :]
            v = qkv[0:upto, v_at:v_at + head]
            scores = contract(q, k, (1, 1))
            rows = lax.broadcasted_iota(jnp.int32, (qb, upto), 0) + i * qb
            scores = jnp.where(rows >= lax.broadcasted_iota(jnp.int32, (qb, upto), 1), scores, -1e30)
            exp_val = jnp.exp(scores - jnp.max(scores, axis=-1, keepdims=True))
            prob = exp_val / jnp.sum(exp_val, axis=-1, keepdims=True)
            prob_b = prob.astype(BF16)
            att[sl, r * head:(r + 1) * head] = contract(prob_b, v, (1, 0)).astype(BF16)
            do = datt[sl, r * head:(r + 1) * head]
            d_prob = contract(do, v, (1, 1)).astype(BF16).astype(F32)
            d_scores = (prob * (d_prob - jnp.sum(d_prob * prob, axis=-1, keepdims=True))).astype(BF16)
            d_rot = contract(d_scores, k, (1, 0)).astype(BF16).astype(F32) * scale
            cos_t, sin_t = cos_of(sl)
            first, second = d_rot[:, 0:half], d_rot[:, half:head]
            dq[sl, r * head:r * head + half] = (first * cos_t + second * sin_t).astype(BF16)
            dq[sl, r * head + half:(r + 1) * head] = (second * cos_t - first * sin_t).astype(BF16)
            dk_acc[0:upto, :] += contract(d_scores, q, (0, 0))
            dv_acc[0:upto, :] += contract(prob_b, do, (0, 0))
    dkv[:, 0:head] = dk_acc[...].astype(BF16)
    dkv[:, head:2 * head] = dv_acc[...].astype(BF16)


def attention_call(qkv, datt, table, n_batch):
    tok, wide = qkv.shape
    inner = datt.shape[1]
    head = table.shape[1]
    n_pos = tok // n_batch
    heads = inner // head

    def rows(n):
        return pl.BlockSpec((n_pos, n), lambda b: (b, 0))

    shape = jax.ShapeDtypeStruct
    flops = 2 * n_batch * heads * n_pos * n_pos * head * 7
    return pl.pallas_call(
        functools.partial(attention_kernel, heads),
        grid=(n_batch,),
        out_shape=(shape((tok, inner), BF16), shape((tok, inner), BF16), shape((tok, 2 * head), BF16)),
        in_specs=[rows(wide), rows(inner), pl.BlockSpec(table.shape, lambda b: (0, 0))],
        out_specs=(rows(inner), rows(inner), rows(2 * head)),
        scratch_shapes=[pltpu.VMEM((n_pos, head), BF16), pltpu.VMEM((n_pos, head), F32), pltpu.VMEM((n_pos, head), F32)],
        cost_estimate=pl.CostEstimate(flops=flops, bytes_accessed=20_000_000, transcendentals=n_batch * heads * n_pos * n_pos),
        compiler_params=pltpu.CompilerParams(vmem_limit_bytes=40_000_000),
        name='attention',
    )(qkv, datt, table)


def solution(mesh):
    def device_step(x_in, dy_out, ln_gain, w_q, w_k, w_v, w_o, w_gate, w_up, w_down):
        n_batch, seq_len, width = x_in.shape
        head_dim = w_k.shape[1]
        inner = w_q.shape[1]
        ff = w_gate.shape[1]
        tok = n_batch * seq_len
        x_rows = x_in.reshape(tok, width)
        dy = dy_out.reshape(tok, width)
        table = jnp.concatenate(rope_tables(seq_len, head_dim), axis=-1)

        gain8 = jnp.broadcast_to(ln_gain[None, :], (8, ln_gain.shape[0]))
        front = front_call(x_rows, dy, gain8, w_q, jnp.concatenate([w_k, w_v], axis=1), w_gate, w_up, jnp.concatenate([w_o, w_down], axis=0))
        wcat, wkv, wod, gain, h_norm, qkv, gate, up, act, d_att, d_act = front
        att, d_q, dkv = attention_call(qkv, d_att, table, n_batch)
        res = back_call(att, act, wod, gate, up, d_act, d_q, wcat, wkv, dkv, table, h_norm, dy, x_rows, gain)
        y_rows, gx_rows = res[0], res[1]
        own_a, own_b, got_a, got_b, gsum, _, kvsum = res[9:16]

        def total(own, got):
            return own + got[0].astype(F32) + got[1].astype(F32) + got[2].astype(F32)

        grad_od = total(own_a, got_a)
        big = 2 * ff + inner
        grad_in = total(own_b[:, :big], got_b[:, :, :big])
        grad_kv = kvsum[0] + kvsum[1]
        grad_gain = gsum[0, 0] + gsum[1, 0]
        return (y_rows.reshape(x_in.shape), gx_rows.reshape(x_in.shape), grad_gain, grad_in[:, 2 * ff:2 * ff + inner],
                grad_kv[:, :head_dim], grad_kv[:, head_dim:], grad_od[:inner], grad_in[:, :ff], grad_in[:, ff:2 * ff], grad_od[inner:])

    act_spec = P('fsdp', None, None)
    row_spec = P('fsdp', 'tp')
    kv_spec = P('fsdp', None)
    col_spec = P('tp', 'fsdp')
    in_specs = (act_spec, act_spec, P('fsdp'), row_spec, kv_spec, kv_spec, col_spec, row_spec, row_spec, col_spec)
    out_specs = (act_spec, act_spec, P('fsdp'), row_spec, kv_spec, kv_spec, col_spec, row_spec, row_spec, col_spec)
    return jax.shard_map(device_step, mesh=mesh, in_specs=in_specs, out_specs=out_specs, check_vma=False)
```

```python
import functools
import math
import jax
import jax.numpy as jnp
from jax import lax
from jax.experimental import pallas as pl
from jax.experimental.pallas import tpu as pltpu
from jax.sharding import PartitionSpec as P

F32 = jnp.float32
BF16 = jnp.bfloat16
WIRE = jnp.bfloat16
STEP = 32
ZERO, ONE, TWO, THREE = range(4)


def rope_tables(seq_len, head_dim):
    half_dim = head_dim // 2
    inv_freq = jnp.power(10000.0, -2.0 * jnp.arange(half_dim, dtype=F32) / head_dim)
    angle = jnp.arange(seq_len, dtype=F32)[:, None] * inv_freq[None, :]
    return jnp.cos(angle), jnp.sin(angle)


def row_loop(rows, fn):
    def body(i, carry):
        fn(pl.ds(pl.multiple_of(i * STEP, STEP), STEP))
        return carry

    lax.fori_loop(0, rows // STEP, body, 0)


def contract(left, right, dims):
    return lax.dot_general(left, right, ((dims[:1], dims[1:]), ((), ())), preferred_element_type=F32)


def front_kernel(dims, x, dy, gain, sq, sk, sv, so, sd, sg, su,
                 wcat, wkv, wod, gain_all, h, qkv, gate, up, act, datt, dact,
                 hv, wv, wodv, wqv, xt, yt, gt, et, b_q, b_k, b_v, b_o, b_d, b_g, b_u, gv,
                 load, wload, keep, bsem, gsem, gain_s, gain_r, send, recv):
    rt_rows, split = dims
    tok, width = x.shape
    inner, head, ff = sq.shape[ONE], sk.shape[ONE], sg.shape[ONE]
    kv = TWO * head
    blk = sq.shape[ZERO]
    ka = inner + ff
    n = tok // rt_rows
    me = lax.axis_index('fsdp')

    def local(src, dst, sem):
        return pltpu.make_async_copy(src, dst, sem)

    def remote(src, dst, s, r, to):
        return pltpu.make_async_remote_copy(src_ref=src, dst_ref=dst, send_sem=s, recv_sem=r, device_id={'fsdp': me ^ to},
                                            device_id_type=pl.DeviceIdType.MESH)

    items = (
        (sq, wcat, TWO * ff, inner, False), (sk, wkv, ZERO, head, False), (sv, wkv, head, head, False),
        (so, wod, ZERO, inner, True), (sd, wod, inner, ff, True), (sg, wcat, ZERO, ff, False), (su, wcat, ff, ff, False),
    )
    group_q, group_o, group_g, group_u = (ZERO, ONE, TWO), (THREE, 4), (5,), (6,)

    def block(i, mask, part=None):
        _, whole_w, at, wide, tall = items[i]
        at_blk = pl.multiple_of((me ^ mask) * blk, blk)
        if tall:
            rows = pl.ds(at, wide) if part is None else pl.ds(at + part * (wide // TWO), wide // TWO)
            return whole_w.at[rows, pl.ds(at_blk, blk)]
        rows = pl.ds(at_blk, blk) if part is None else pl.ds(at_blk + part * (blk // TWO), blk // TWO)
        return whole_w.at[rows, pl.ds(at, wide)]

    def own_to(i, to, num):
        return remote(items[i][ZERO], block(i, ZERO), send.at[i, num], recv.at[i, num], to)

    def pass_to(i, mask, to, num, part=None):
        return remote(block(i, mask, part), block(i, mask, part), send.at[i, num], recv.at[i, num], to)

    def arrived(i, mask, to, num, part=None):
        remote(block(i, mask, part), block(i, mask, part), send.at[i, num], recv.at[i, num], to).wait_recv()

    def depart(group):
        for i in group:
            own_to(i, TWO, ZERO).start()
            own_to(i, 4, ONE).start()
            own_to(i, ONE, 4).start()

    def relay(group):
        for i in group:
            arrived(i, TWO, TWO, ZERO)
            pass_to(i, TWO, 4, TWO, ZERO).start()
            arrived(i, 4, 4, ONE)
            pass_to(i, 4, TWO, THREE, ONE).start()
            pass_to(i, TWO, ONE, 5).start()
            pass_to(i, 4, ONE, 6).start()

    def corner(group):
        for i in group:
            arrived(i, 6, 4, TWO, ZERO)
            pass_to(i, 6, ONE, 7, ZERO).start()
            arrived(i, 6, TWO, THREE, ONE)
            pass_to(i, 6, ONE, 8, ONE).start()

    def full(group):
        for i in group:
            arrived(i, ONE, ONE, 4)
            arrived(i, THREE, ONE, 5)
            arrived(i, 5, ONE, 6)
            arrived(i, 7, ONE, 7, ZERO)
            arrived(i, 7, ONE, 8, ONE)

    def sent(i):
        own_to(i, TWO, ZERO).wait_send()
        own_to(i, 4, ONE).wait_send()
        own_to(i, ONE, 4).wait_send()
        pass_to(i, TWO, 4, TWO, ZERO).wait_send()
        pass_to(i, 4, TWO, THREE, ONE).wait_send()
        pass_to(i, TWO, ONE, 5).wait_send()
        pass_to(i, 4, ONE, 6).wait_send()
        pass_to(i, 6, ONE, 7, ZERO).wait_send()
        pass_to(i, 6, ONE, 8, ONE).wait_send()

    bounce = (b_q, b_k, b_v, b_o, b_d, b_g, b_u)

    def own_in(i):
        return local(items[i][ZERO], bounce[i], bsem.at[i])

    def own_out(i):
        return local(bounce[i], block(i, ZERO), bsem.at[i])

    def tile_rows(k):
        return pl.ds(pl.multiple_of(k * rt_rows, rt_rows), rt_rows)

    def tiles(fn):
        def body(k, carry):
            fn(k)
            return carry

        lax.fori_loop(ZERO, n, body, ZERO)

    def dot_cols(left, weight, dims_, out, wide):
        col = wide // split

        def body(j, carry):
            cs = pl.ds(pl.multiple_of(j * col, col), col)
            rhs = weight[:, cs] if dims_[ONE] == ZERO else weight[cs, :]
            out[:, cs] = contract(left[...], rhs, dims_).astype(BF16)
            return carry

        lax.fori_loop(ZERO, split, body, ZERO)

    def gain_cols(mask):
        return pl.ds(pl.multiple_of((me ^ mask) * blk, blk), blk)

    def gain_to(m):
        return remote(gain, gain_all.at[:, gain_cols(ZERO)], gain_s.at[m - ONE], gain_r.at[m - ONE], m)

    def gain_from(m):
        return remote(gain, gain_all.at[:, gain_cols(m)], gain_s.at[m - ONE], gain_r.at[m - ONE], m)

    def gain_in(m):
        return local(gain if m == ZERO else gain_all.at[:, gain_cols(m)], gv.at[:, gain_cols(m)], gsem.at[m])

    peers = range(ONE, 8)
    for m in peers:
        gain_to(m).start()
    depart(group_q)
    gain_in(ZERO).start()
    n_items = len(items)
    for i in range(n_items):
        own_in(i).start()
    for m in peers:
        gain_from(m).wait_recv()
        gain_in(m).start()
    for i in range(n_items):
        own_in(i).wait()
        own_out(i).start()
    for m in range(8):
        gain_in(m).wait()

    def x_load(k):
        return local(x.at[tile_rows(k)], xt.at[lax.rem(k, TWO)], load.at[lax.rem(k, TWO)])

    def h_keep(k):
        return local(hv.at[tile_rows(k)], h.at[tile_rows(k)], keep.at[lax.rem(k, TWO)])

    x_load(ZERO).start()

    def norm(k):
        x_load(k).wait()

        @pl.when(k + ONE < n)
        def _():
            x_load(k + ONE).start()

        def rows(sl):
            xv = xt[lax.rem(k, TWO), sl, :].astype(F32)
            cent = xv - jnp.mean(xv, axis=-ONE, keepdims=True)
            inv = lax.rsqrt(jnp.mean(cent * cent, axis=-ONE, keepdims=True) + 1e-5)
            hv[pl.ds(pl.multiple_of(k * rt_rows + sl.start, STEP), STEP), :] = (cent * inv * gv[ZERO:ONE, :]).astype(BF16)

        row_loop(rt_rows, rows)

        @pl.when(k >= TWO)
        def _():
            h_keep(k - TWO).wait()

        h_keep(k).start()

        @pl.when(k == n // TWO)
        def _():
            relay(group_q)
            depart(group_o)

    tiles(norm)
    h_keep(n - TWO).wait()
    h_keep(n - ONE).wait()

    corner(group_q)
    for i in range(n_items):
        own_out(i).wait()
    full(group_q)
    w0 = local(wcat.at[:, pl.ds(TWO * ff, inner)], wqv.at[:, pl.ds(ZERO, inner)], wload.at[ZERO])
    w1 = local(wkv, wqv.at[:, pl.ds(inner, kv)], wload.at[ONE])
    w0.start()
    w1.start()
    w0.wait()
    w1.wait()

    def after_store(k, copies):
        @pl.when(k >= TWO)
        def _():
            for c in copies(k - TWO):
                c.wait()

    def stored(copies):
        for k in range(max(n - TWO, ZERO), n):
            for c in copies(k):
                c.wait()

    def half(ref, k, at, wide):
        return ref.at[lax.rem(k, TWO), :, pl.ds(at, wide)]

    def qkv_keep(k):
        return (local(half(yt, k, ZERO, inner + kv), qkv.at[tile_rows(k)], keep.at[lax.rem(k, TWO)]),)

    def qkv_tile(k):
        after_store(k, qkv_keep)
        dot_cols(hv.at[tile_rows(k)], wqv, (ONE, ZERO), yt.at[lax.rem(k, TWO)], inner + kv)
        for c in qkv_keep(k):
            c.start()

    tiles(qkv_tile)
    stored(qkv_keep)

    def dy_load(k):
        return local(dy.at[tile_rows(k)], xt.at[lax.rem(k, TWO)], load.at[lax.rem(k, TWO)])

    dy_load(ZERO).start()
    relay(group_o)
    depart(group_g)
    corner(group_o)
    full(group_o)
    w2 = local(wod, wodv, wload.at[TWO])
    w2.start()
    w2.wait()

    def back_keep(k):
        return (local(half(yt, k, ZERO, inner), datt.at[tile_rows(k)], keep.at[lax.rem(k, TWO)]),
                local(half(yt, k, inner, ff), dact.at[tile_rows(k)], keep.at[TWO + lax.rem(k, TWO)]))

    def back_tile(k):
        dy_load(k).wait()

        @pl.when(k + ONE < n)
        def _():
            dy_load(k + ONE).start()

        after_store(k, back_keep)
        dot_cols(xt.at[lax.rem(k, TWO)], wodv, (ONE, ONE), yt.at[lax.rem(k, TWO)], ka)
        for c in back_keep(k):
            c.start()

        @pl.when(k == n // TWO)
        def _():
            relay(group_g)
            depart(group_u)

    tiles(back_tile)
    stored(back_keep)

    corner(group_g)
    full(group_g)
    w3 = local(wcat.at[:, pl.ds(ZERO, ff)], wv, wload.at[THREE])
    w3.start()
    w3.wait()

    def gate_keep(k):
        return (local(half(yt, k, ZERO, ff), gate.at[tile_rows(k)], keep.at[lax.rem(k, TWO)]),)

    def gate_tile(k):
        after_store(k, gate_keep)
        dot_cols(hv.at[tile_rows(k)], wv, (ONE, ZERO), yt.at[lax.rem(k, TWO)], ff)
        for c in gate_keep(k):
            c.start()

        @pl.when(k == n // TWO)
        def _():
            relay(group_u)

    tiles(gate_tile)
    stored(gate_keep)

    def gate_load(k):
        return local(gate.at[tile_rows(k)], gt, load.at[TWO])

    gate_load(ZERO).start()
    corner(group_u)
    full(group_u)
    w4 = local(wcat.at[:, pl.ds(ff, ff)], wv, wload.at[4])
    w4.start()
    w4.wait()

    def up_keep(k):
        return (local(half(yt, k, ZERO, ff), up.at[tile_rows(k)], keep.at[lax.rem(k, TWO)]),
                local(et.at[lax.rem(k, TWO)], act.at[tile_rows(k)], keep.at[TWO + lax.rem(k, TWO)]))

    def up_tile(k):
        after_store(k, up_keep)
        dot_cols(hv.at[tile_rows(k)], wv, (ONE, ZERO), yt.at[lax.rem(k, TWO)], ff)
        gate_load(k).wait()

        def rows(sl):
            g = gt[sl, :].astype(F32)
            et[lax.rem(k, TWO), sl, :] = (g * jax.nn.sigmoid(g) * yt[lax.rem(k, TWO), sl, ZERO:ff].astype(F32)).astype(BF16)

        row_loop(rt_rows, rows)

        @pl.when(k + ONE < n)
        def _():
            gate_load(k + ONE).start()

        for c in up_keep(k):
            c.start()

    tiles(up_tile)
    stored(up_keep)
    for i in range(n_items):
        sent(i)
    for m in peers:
        gain_to(m).wait_send()
    g_out = local(gv.at[:, gain_cols(ZERO)], gain_all.at[:, gain_cols(ZERO)], gsem.at[ZERO])
    g_out.start()
    g_out.wait()


def front_call(x, dy, gain, shards, rt_rows=384, split=2):
    sq, sk, sv, so, sd, sg, su = shards
    tok, width = x.shape
    inner, ff = sq.shape[1], sg.shape[1]
    kv = 2 * sk.shape[1]
    ka = inner + ff
    blk = sq.shape[0]
    shape = jax.ShapeDtypeStruct
    outs = (
        shape((width, 2 * ff + inner), BF16), shape((width, kv), BF16), shape((ka, width), BF16), shape((8, width), F32),
        shape((tok, width), BF16), shape((tok, inner + kv), BF16), shape((tok, ff), BF16), shape((tok, ff), BF16), shape((tok, ff), BF16),
        shape((tok, inner), BF16), shape((tok, ff), BF16),
    )
    sems = pltpu.SemaphoreType.DMA
    scratch = [
        pltpu.VMEM((tok, width), BF16), pltpu.VMEM((width, ff), BF16), pltpu.VMEM((ka, width), BF16), pltpu.VMEM((width, inner + kv), BF16),
        pltpu.VMEM((2, rt_rows, width), BF16), pltpu.VMEM((2, rt_rows, max(ka, inner + kv)), BF16), pltpu.VMEM((rt_rows, ff), BF16),
        pltpu.VMEM((2, rt_rows, ff), BF16), *[pltpu.VMEM(w.shape, BF16) for w in shards],
        pltpu.VMEM((8, width), F32),
        sems((3,)), sems((5,)), sems((4,)), sems((7,)), sems((8,)), sems((7,)), sems((7,)), sems((7, 9)), sems((7, 9)),
    ]
    flops = 2 * tok * width * (2 * ka + ff + kv)
    anywhere = pl.BlockSpec(memory_space=pl.ANY)
    return pl.pallas_call(
        functools.partial(front_kernel, (rt_rows, split)),
        out_shape=outs,
        in_specs=[anywhere] * 10,
        out_specs=tuple(anywhere for _ in outs),
        scratch_shapes=scratch,
        cost_estimate=pl.CostEstimate(flops=flops, bytes_accessed=150_000_000, transcendentals=tok * ff),
        compiler_params=pltpu.CompilerParams(vmem_limit_bytes=67_000_000, has_side_effects=True),
        name='forward',
    )(x, dy, gain, *shards)


def back_kernel(dims, att, act, wod, gate, up, dact, dq, wcat, wkv, dkv, table, h, dy, x, gain,
                y_out, gx_out, part, line, kvline, dcat, dhkv, peer_a, peer_b, own_a, own_b, got_a, got_b, gsum, gtmp, kvsum, snd_a, snd_b,
                wa, wb, st, wv, tv, ctile, gt, ot, rt, sa, sb, zr, zo, zs, zx, zd, zk, kr, ko, kz, gv, kw, gw,
                load, wload, wait_y, zload, zstore, kstore, rs_s, rs_r, kv_s, kv_r, ag_s, ag_r, core_s, core_r, far_s, far_r, own_s, put_s, kf_s, kf_r, kf_l, gl_s, gf_s, gf_r, gz_s, gz_r):
    nc, cr, col, tile = dims
    tok, width = h.shape
    inner, ff = att.shape[ONE], act.shape[ONE]
    ka, kb = inner + ff, wcat.shape[ONE]
    kv = dkv.shape[ONE]
    head = kv // TWO
    n_pos = table.shape[ZERO]
    rt_rows = 4 * cr
    blk = width // 8
    mid = width // TWO
    na, nb = ka // tile, (kb + kv) // tile
    depth = THREE
    last = THREE
    hop_lag = TWO
    end = TWO * nc - ONE + hop_lag * (last + TWO)
    me = lax.axis_index('fsdp')
    z = lax.axis_index('tp')

    def remote(src, dst, send, recv, **to):
        return pltpu.make_async_remote_copy(src_ref=src, dst_ref=dst, send_sem=send, recv_sem=recv,
                                            device_id=to, device_id_type=pl.DeviceIdType.MESH)

    def local(src, dst, sem):
        return pltpu.make_async_copy(src, dst, sem)

    def chunk_row(d, c):
        return pl.multiple_of(lax.rem(c, nc) * (TWO * cr) + d * cr, cr)

    def chunk_rows(d, c):
        return pl.ds(chunk_row(d, c), cr)

    def slot_parts(t):
        parts = []
        up_z, down_z = lax.rem(z + ONE, last + ONE), lax.rem(z + last, last + ONE)
        for d in range(TWO):
            parts.append(line_parts(t, d, up_z, down_z))
        return parts

    def line_parts(t, d, up_z, down_z):
        if True:
            rank = z if d == ZERO else last - z
            fwd, back = (up_z, down_z) if d == ZERO else (down_z, up_z)

            def hop(c, src=None):
                src = part.at[lax.div(c, nc), chunk_rows(d, c)] if src is None else src
                return remote(src, line.at[d, c], rs_s.at[d, c], rs_r.at[d, c], tp=fwd)

            def mid_hop(c):
                return hop(c, zs.at[d, lax.rem(c, depth)])

            def kv_hop(c, src=None):
                src = dkv.at[chunk_rows(d, c)] if src is None else src
                return remote(src, kvline.at[d, c], kv_s.at[d, c], kv_r.at[d, c], tp=fwd)

            def mid_kv_hop(c):
                return kv_hop(c, kz.at[d, lax.rem(c, depth)])

            def bcast_of(c, dst, src=None):
                src = dst.at[chunk_rows(d, c)] if src is None else src
                return remote(src, dst.at[chunk_rows(d, c)], ag_s.at[d, c], ag_r.at[d, c], tp=back)

            def keep_of(c, dst):
                return local(zs.at[d, lax.rem(c, depth)], dst.at[chunk_rows(d, c)], zstore.at[d, lax.rem(c, depth)])

            def for_kind(c, fn):
                @pl.when(c < nc)
                def _():
                    fn(y_out)

                @pl.when(c >= nc)
                def _():
                    fn(gx_out)

            def depart():
                @pl.when((rank == ZERO) & (t >= ZERO) & (t < TWO * nc))
                def _():
                    hop(t).start()

                    @pl.when(t < nc)
                    def _():
                        kv_hop(t).start()

            c = t - hop_lag * rank
            rows = chunk_rows(d, c)
            own = pl.ds(pl.multiple_of(lax.rem(c, nc) * cr, cr), cr)

            def load_of(i):
                return (
                    local(part.at[lax.div(c, nc), rows], zo.at[d], zload.at[d, ZERO]), local(line.at[d, c], zr.at[d], zload.at[d, ONE]),
                    local(x.at[rows], zx, zload.at[d, TWO]), local(dy.at[rows], zd, zload.at[d, THREE]),
                    local(dhkv.at[own], zk, zload.at[d, 4]), local(dkv.at[rows], ko.at[d], zload.at[d, 5]),
                    local(kvline.at[d, lax.rem(c, nc)], kr.at[d], zload.at[d, 6]),
                )[i]

            busy = (rank > ZERO) & (c >= ZERO) & (c < TWO * nc)

            def begin():
                @pl.when(busy)
                def _():
                    load_of(ZERO).start()

                    @pl.when(rank == last)
                    def _():
                        load_of(TWO).start()

                        @pl.when(c >= nc)
                        def _():
                            load_of(THREE).start()

                    hop(c).wait_recv()
                    load_of(ONE).start()

                    @pl.when(c < nc)
                    def _():
                        load_of(5).start()
                        kv_hop(c).wait_recv()
                        load_of(6).start()

            def finish():
                @pl.when(busy & (rank < last))
                def _():
                    @pl.when(c >= depth)
                    def _():
                        mid_hop(c - depth).wait_send()

                    load_of(ZERO).wait()
                    load_of(ONE).wait()

                    def add(sl):
                        zs[d, lax.rem(c, depth), sl, :] = (zr[d, sl, :].astype(F32) + zo[d, sl, :].astype(F32)).astype(BF16)

                    row_loop(cr, add)
                    mid_hop(c).start()

                    @pl.when(c < nc)
                    def _():
                        @pl.when(c >= depth)
                        def _():
                            mid_kv_hop(c - depth).wait_send()

                        load_of(5).wait()
                        load_of(6).wait()
                        kz[d, lax.rem(c, depth)] = (kr[d].astype(F32) + ko[d].astype(F32)).astype(BF16)
                        mid_kv_hop(c).start()

                @pl.when(busy & (rank == last))
                def _():
                    @pl.when(c >= nc)
                    def _():
                        load_of(4).start()

                    @pl.when(c >= depth)
                    def _():
                        bcast_of(c - depth, y_out).wait_send()
                        keep_of(c - depth, y_out).wait()

                    load_of(ZERO).wait()
                    load_of(ONE).wait()
                    load_of(TWO).wait()

                    @pl.when(c < nc)
                    def _():
                        def fin(sl):
                            branch = zr[d, sl, :].astype(F32) + zo[d, sl, :].astype(F32)
                            zs[d, lax.rem(c, depth), sl, :] = (zx[sl, :].astype(F32) + branch).astype(BF16)

                        row_loop(cr, fin)

                    @pl.when(c >= nc)
                    def _():
                        load_of(THREE).wait()
                        load_of(4).wait()

                        def fin(sl):
                            dh = (zr[d, sl, :].astype(F32) + zo[d, sl, :].astype(F32) + zk[sl, :]).astype(BF16).astype(F32)
                            xv = zx[sl, :].astype(F32)
                            cent = xv - jnp.mean(xv, axis=-ONE, keepdims=True)
                            inv = lax.rsqrt(jnp.mean(cent * cent, axis=-ONE, keepdims=True) + 1e-5)
                            hat = cent * inv
                            gv[8:9, :] = gv[8:9, :] + jnp.sum(dh * hat, axis=ZERO, keepdims=True)
                            dn = dh * gv[ZERO:ONE, :]
                            dx = inv * (dn - jnp.mean(dn, axis=-ONE, keepdims=True)
                                        - hat * jnp.mean(dn * hat, axis=-ONE, keepdims=True))
                            zs[d, lax.rem(c, depth), sl, :] = (zd[sl, :].astype(F32) + dx).astype(BF16)

                        row_loop(cr, fin)

                    for_kind(c, lambda dst: keep_of(c, dst).start())
                    for_kind(c, lambda dst: bcast_of(c, dst, zs.at[d, lax.rem(c, depth)]).start())

                    @pl.when(c < nc)
                    def _():
                        load_of(5).wait()
                        load_of(6).wait()
                        pos = pl.ds(pl.multiple_of(lax.rem(chunk_row(d, c), n_pos), cr), cr)
                        cos_t, sin_t = tv[pos, ZERO:head // TWO], tv[pos, head // TWO:head]

                        def summed(lo, hi):
                            return (kr[d, :, lo:hi].astype(F32) + ko[d, :, lo:hi].astype(F32)).astype(BF16)

                        first = summed(ZERO, head // TWO).astype(F32)
                        second = summed(head // TWO, head).astype(F32)
                        kz[d, ZERO, :, ZERO:head // TWO] = (first * cos_t + second * sin_t).astype(BF16)
                        kz[d, ZERO, :, head // TWO:head] = (second * cos_t - first * sin_t).astype(BF16)
                        kz[d, ZERO, :, head:kv] = summed(head, kv)
                        keep_kv = local(kz.at[d, ZERO], dcat.at[rows, pl.ds(kb, kv)], kstore.at[ZERO])
                        keep_kv.start()

                        def cols(j, carry):
                            cs = pl.ds(pl.multiple_of(j * col, col), col)
                            zk[:, cs] = contract(kz[d, ZERO], wv[cs, :], (ONE, ONE))
                            return carry

                        lax.fori_loop(ZERO, width // col, cols, ZERO)
                        keep_h = local(zk, dhkv.at[own], kstore.at[ONE])
                        keep_h.start()
                        keep_kv.wait()
                        keep_h.wait()

            e = t - hop_lag * (last + ONE) - hop_lag * (TWO - rank)

            def pass_on():
                @pl.when(((rank == ONE) | (rank == TWO)) & (e >= ZERO) & (e < TWO * nc))
                def _():
                    bcast_of(e, y_out).wait_recv()
                    for_kind(e, lambda dst: bcast_of(e, dst).start())

            def settle():
                def each(c, carry):
                    tail = TWO * nc - depth
                    kv_tail = (c >= nc - depth) & (c < nc)

                    @pl.when(rank == ZERO)
                    def _():
                        hop(c).wait_send()
                        bcast_of(c, y_out).wait_recv()

                        @pl.when(c < nc)
                        def _():
                            kv_hop(c).wait_send()

                    @pl.when((rank == ONE) | (rank == TWO))
                    def _():
                        bcast_of(c, y_out).wait_send()

                        @pl.when(c >= tail)
                        def _():
                            mid_hop(c).wait_send()

                        @pl.when(kv_tail)
                        def _():
                            mid_kv_hop(c).wait_send()

                    @pl.when((rank == last) & (c >= tail))
                    def _():
                        bcast_of(c, y_out).wait_send()
                        keep_of(c, y_out).wait()

                    return carry

                lax.fori_loop(ZERO, TWO * nc, each, ZERO)

            return depart, begin, finish, pass_on, settle

    def slot(t):
        parts = slot_parts(t)
        for i in range(4):
            for p in parts:
                p[i]()

        @pl.when(t == end)
        def _():
            for p in parts:
                p[4]()

    def gain_total():
        low = pl.ds(8, 8)
        which = lax.div(z, last)

        def cols(mask):
            return pl.ds(pl.multiple_of((me ^ mask) * blk, blk), blk)

        def plane(m):
            return remote(gv.at[low, cols(m)], gtmp.at[m], gf_s.at[m], gf_r.at[m], fsdp=me ^ m)

        def along(i):
            return remote(gw.at[ZERO], gsum.at[which], gz_s.at[i], gz_r.at[which], tp=lax.rem(z + ONE + i, last + ONE))

        def arrived(w):
            remote(gw.at[ZERO], gsum.at[w], gz_s.at[ZERO], gz_r.at[w], tp=lax.rem(z + ONE, last + ONE)).wait_recv()

        peers = range(ONE, 8)

        @pl.when((z == ZERO) | (z == last))
        def _():
            for m in peers:
                plane(m).start()
            own = local(gv.at[low, cols(ZERO)], gw.at[ZERO], gl_s.at[ZERO])
            own.start()
            for m in peers:
                plane(m).wait_recv()
                local(gtmp.at[m], gw.at[m], gl_s.at[m]).start()
            own.wait()
            for m in peers:
                local(gtmp.at[m], gw.at[m], gl_s.at[m]).wait()
            gw[ZERO] = jnp.sum(gw[...], axis=ZERO)
            home = local(gw.at[ZERO], gsum.at[which], gl_s.at[ZERO])
            home.start()
            for i in range(THREE):
                along(i).start()
            home.wait()
            for m in peers:
                plane(m).wait_send()

        @pl.when(z != ZERO)
        def _():
            arrived(ZERO)

        @pl.when(z != last)
        def _():
            arrived(ONE)

        @pl.when((z == ZERO) | (z == last))
        def _():
            for i in range(THREE):
                along(i).wait_send()

    def tile_rows(k):
        return pl.ds(pl.multiple_of(k * rt_rows, rt_rows), rt_rows)

    def y_step(k):
        srcs = [local(att.at[tile_rows(k)], ctile.at[:, pl.ds(ZERO, inner)], load.at[ZERO]),
                local(act.at[tile_rows(k)], ctile.at[:, pl.ds(inner, ff)], load.at[ONE])]
        for s in srcs:
            s.start()
        for s in srcs:
            s.wait()

        def cols(j, carry):
            cs = pl.ds(pl.multiple_of(j * col, col), col)
            gt[:, cs] = contract(ctile[:, ZERO:ka], wa[ZERO:ka, cs], (ONE, ZERO)).astype(BF16)
            return carry

        lax.fori_loop(ZERO, width // col, cols, ZERO)
        dst = local(gt.at[:, pl.ds(ZERO, width)], part.at[ZERO, tile_rows(k)], wait_y)
        dst.start()
        dst.wait()

    def h_step(k):
        rows = tile_rows(k)
        srcs = [local(gate.at[rows], gt.at[:, pl.ds(ZERO, ff)], load.at[ZERO]), local(up.at[rows], ctile.at[:, pl.ds(ZERO, ff)], load.at[ONE]),
                local(dact.at[rows], ctile.at[:, pl.ds(ff, ff)], load.at[TWO]), local(dq.at[rows], ctile.at[:, pl.ds(TWO * ff, kb - TWO * ff)], load.at[THREE])]
        for s in srcs:
            s.start()
        for s in srcs:
            s.wait()

        def act_back(sl):
            g = gt[sl, ZERO:ff].astype(F32)
            u = ctile[sl, ZERO:ff].astype(F32)
            d_act = ctile[sl, ff:TWO * ff].astype(F32)
            sig = jax.nn.sigmoid(g)
            ctile[sl, ZERO:ff] = (d_act * u * (sig + g * sig * (1.0 - sig))).astype(BF16)
            ctile[sl, ff:TWO * ff] = (d_act * (g * sig)).astype(BF16)

        row_loop(rt_rows, act_back)
        keep = local(ctile, dcat.at[rows, pl.ds(ZERO, kb)], load.at[4])
        keep.start()

        def cols(j, carry):
            cs = pl.ds(pl.multiple_of(j * col, col), col)
            gt[:, cs] = contract(ctile[...], wb[cs, ZERO:kb], (ONE, ONE)).astype(BF16)
            return carry

        lax.fori_loop(ZERO, width // col, cols, ZERO)
        dst = local(gt.at[:, pl.ds(ZERO, width)], part.at[ONE, rows], wait_y)
        dst.start()
        dst.wait()
        keep.wait()

    def out_weights():
        return local(wod, wa.at[pl.ds(ZERO, ka)], wload.at[ZERO])

    def in_weights():
        return local(wcat, wb.at[pl.ds(ZERO, width), pl.ds(ZERO, kb)], wload.at[10])

    def operand(src):
        cps = []
        for q in range(8):
            mask = TWO * (q % 4) + q // 4
            cols = pl.ds(pl.multiple_of((me ^ mask) * blk, blk), blk)
            cps.append(local(src.at[:, cols], wa.at[pl.ds(ZERO, tok), pl.ds(q * blk, blk)], wload.at[q]))
        for c in cps:
            c.start()
        for c in cps:
            c.wait()

    first_b = -(-nb // TWO)

    def strip(is_a, k):
        if is_a:
            return k
        return jnp.where(k < first_b, k, jnp.where(k == first_b, nb - ONE, k - ONE))

    def wide_start(is_a, k):
        dst = st.at[lax.rem(k, TWO)]
        sem = wload.at[8 + lax.rem(k, TWO)]
        if is_a:
            @pl.when(k == ZERO)
            def _():
                local(att, dst, sem).start()

            @pl.when(k > ZERO)
            def _():
                local(act.at[:, pl.ds(pl.multiple_of((k - ONE) * tile, tile), tile)], dst, sem).start()
        else:
            local(dcat.at[:, pl.ds(pl.multiple_of(strip(is_a, k) * tile, tile), tile)], dst, sem).start()

    def wide(is_a, k, hi):
        local(dcat.at[:, pl.ds(ZERO, tile)], st.at[lax.rem(k, TWO)], wload.at[8 + lax.rem(k, TWO)]).wait()

        @pl.when(k + ONE < hi)
        def _():
            wide_start(is_a, k + ONE)

    def prod(is_a, k, odd):
        half = pl.ds(odd * mid, mid)
        if is_a:
            return contract(st[lax.rem(k, TWO)], wa[ZERO:tok, half], (ZERO, ZERO))
        return contract(wa[ZERO:tok, half], st[lax.rem(k, TWO)], (ZERO, ZERO))

    def place(ref, is_a, k):
        par = pl.multiple_of(lax.rem(k, TWO) * tile, tile)
        return ref.at[pl.ds(par, tile), :] if is_a else ref.at[:, pl.ds(par, tile)]

    def whole(ref, is_a, k):
        cs = pl.ds(pl.multiple_of(strip(is_a, k) * tile, tile), tile)
        return ref.at[cs, :] if is_a else ref.at[:, cs]

    def piece(ref, is_a, q):
        return ref.at[:, pl.ds(q * blk, blk)] if is_a else ref.at[pl.ds(q * blk, blk), :]

    def away(is_a, k, q):
        base, snd, got = (ZERO, snd_a, got_a) if is_a else (na, snd_b, got_b)
        return remote(whole(snd.at[q], is_a, k), whole(got.at[q], is_a, k), far_s.at[q, base + k], far_r.at[q, base + k],
                      fsdp=me ^ (TWO * (q + ONE)))

    def odd_steps(is_a, lo, hi, stop):
        base = ZERO if is_a else na
        peer = peer_a if is_a else peer_b

        def send(k):
            return remote(place(ot, is_a, k), whole(peer, is_a, k), core_s.at[base + k], core_r.at[base + k], fsdp=me ^ ONE)

        def one(k, carry):
            wide(is_a, k, hi)

            @pl.when(k >= stop[ZERO] + TWO)
            def _():
                send(k - TWO).wait_send()

            place(ot, is_a, k)[...] = prod(is_a, k, ONE)
            send(k).start()

            @pl.when(k == stop[ONE] - ONE)
            def _():
                send(k - ONE).wait_send()
                send(k).wait_send()

            return carry

        wide_start(is_a, lo)
        lax.fori_loop(lo, hi, one, ZERO)

    def even_steps(is_a, lo, hi, stop):
        base = ZERO if is_a else na
        peer, own, snd = (peer_a, own_a, snd_a) if is_a else (peer_b, own_b, snd_b)
        stage = sa if is_a else sb

        def take(k):
            return remote(place(ot, is_a, k), whole(peer, is_a, k), core_s.at[base + k], core_r.at[base + k], fsdp=me ^ ONE)

        def fetch(k):
            if not is_a:
                return [local(whole(peer, is_a, k), rt, own_s.at[TWO])]
            rows = pl.ds(pl.multiple_of(k * tile, tile), tile)
            return [local(peer.at[rows, pl.ds(i * tile, tile)], rt.at[pl.ds(i * tile, tile)], own_s.at[TWO + i])
                    for i in range(mid // tile)]

        def fetched():
            if not is_a:
                return rt[...]
            return jnp.concatenate([rt[i * tile:(i + ONE) * tile, :] for i in range(mid // tile)], axis=ONE)

        def mine(k):
            return local(piece(place(ot, is_a, k), is_a, ZERO), whole(own, is_a, k), own_s.at[lax.rem(k, TWO)])

        def put(k, q):
            return local(stage.at[lax.rem(k, TWO), q], whole(snd.at[q], is_a, k), put_s.at[lax.rem(k, TWO), q])

        def ship(k):
            for q in range(THREE):
                put(k, q).wait()
                away(is_a, k, q).start()

        def one(k, carry):
            take(k).wait_recv()
            for f in fetch(k):
                f.start()
            wide(is_a, k, hi)

            @pl.when(k >= stop[ZERO] + TWO)
            def _():
                mine(k - TWO).wait()

            acc = prod(is_a, k, ZERO)

            @pl.when(k >= stop[ZERO] + ONE)
            def _():
                ship(k - ONE)

            for f in fetch(k):
                f.wait()
            place(ot, is_a, k)[...] = acc + fetched()
            mine(k).start()
            for q in range(THREE):
                stage[lax.rem(k, TWO), q] = piece(place(ot, is_a, k), is_a, q + ONE)[...].astype(WIRE)
                put(k, q).start()

            @pl.when(k == stop[ONE] - ONE)
            def _():
                ship(k)
                mine(k - ONE).wait()
                mine(k).wait()

            return carry

        wide_start(is_a, lo)
        lax.fori_loop(lo, hi, one, ZERO)

    def far_wait(is_a, k):
        for q in range(THREE):
            away(is_a, k, q).wait_recv()

    def far_waits(is_a, but=-ONE):
        def one(k, carry):
            for q in range(THREE):
                away(is_a, k, q).wait_send()

            @pl.when(k != but)
            def _():
                far_wait(is_a, k)

            return carry

        lax.fori_loop(ZERO, na if is_a else nb, one, ZERO)

    def kv_send(i):
        which = lax.div(z, last)
        return remote(kw, kvsum.at[which], kf_s.at[i], kf_r.at[which], tp=lax.rem(z + ONE + i, last + ONE))

    def kv_total():
        @pl.when((z == ZERO) | (z == last))
        def _():
            k = first_b
            cs = pl.ds((nb - ONE) * tile, tile)
            far_wait(False, k)
            own_cp = local(own_b.at[:, cs], kw, load.at[ZERO])
            cps = [local(got_b.at[q, :, cs], sb.at[ZERO, q], load.at[ONE + q]) for q in range(THREE)]
            own_cp.start()
            for cp in cps:
                cp.start()
            own_cp.wait()
            for cp in cps:
                cp.wait()
            kw[...] = kw[...] + sb[ZERO, ZERO].astype(F32) + sb[ZERO, ONE].astype(F32) + sb[ZERO, TWO].astype(F32)
            home = local(kw, kvsum.at[lax.div(z, last)], kf_l)
            home.start()
            for i in range(THREE):
                kv_send(i).start()
            home.wait()

        @pl.when((z != ZERO) & (z != last))
        def _():
            far_wait(False, first_b)

    def kv_settle():
        def arrived(which):
            remote(kw, kvsum.at[which], kf_s.at[ZERO], kf_r.at[which], tp=lax.rem(z + ONE, last + ONE)).wait_recv()

        @pl.when(z != ZERO)
        def _():
            arrived(ZERO)

        @pl.when(z != last)
        def _():
            arrived(ONE)

        @pl.when((z == ZERO) | (z == last))
        def _():
            for i in range(THREE):
                kv_send(i).wait_send()

    out_weights().start()
    gv[8:16, :] = jnp.zeros((8, width), F32)
    small = [local(gain, gv.at[pl.ds(ZERO, 8)], load.at[ZERO]), local(wkv, wv, load.at[ONE]), local(table, tv, load.at[TWO])]
    for s in small:
        s.start()

    ctile[:, ZERO:kv] = jnp.zeros((rt_rows, kv), BF16)
    blanks = [local(ctile.at[:, pl.ds(ZERO, kv)], dcat.at[pl.ds(i * rt_rows, rt_rows), pl.ds(kb, kv)], wload.at[TWO + i])
              for i in range(nc // TWO)]
    for s in blanks:
        s.start()
    for s in blanks + small:
        s.wait()

    steps = nc // TWO
    a_at, h_at, b_at = steps, steps + 4, TWO * steps + 4
    kv_at = b_at + 10
    per_a, per_b = -(-na // TWO), -(-first_b // TWO)

    def share(at, lo, hi, per, i):
        return jnp.minimum(lo + i * per, hi), jnp.minimum(lo + (i + ONE) * per, hi)

    def phase(s, at, n):
        return pl.when((s >= at) & (s < at + n))

    def step(s, carry):
        slot(s - ONE)

        @phase(s, ZERO, steps)
        def _():
            @pl.when(s == ZERO)
            def _():
                out_weights().wait()
                in_weights().start()

            y_step(s)

        @phase(s, a_at, TWO)
        def _():
            @pl.when(s == a_at)
            def _():
                operand(dy)

            odd_steps(True, *share(s, ZERO, na, per_a, s - a_at), (ZERO, na))

        @phase(s, a_at + TWO, TWO)
        def _():
            even_steps(True, *share(s, ZERO, na, per_a, s - (a_at + TWO)), (ZERO, na))

        @phase(s, h_at, steps)
        def _():
            @pl.when(s == h_at)
            def _():
                in_weights().wait()

            h_step(s - h_at)

        for part_b in range(TWO):
            lo, hi = (ZERO, first_b) if part_b == ZERO else (first_b, nb)
            at = b_at + 4 * part_b

            @phase(s, at, TWO)
            def _():
                if part_b == ZERO:
                    @pl.when(s == at)
                    def _():
                        operand(h)

                odd_steps(False, *share(s, lo, hi, per_b, s - at), (lo, hi))

            @phase(s, at + TWO, TWO)
            def _():
                even_steps(False, *share(s, lo, hi, per_b, s - (at + TWO)), (lo, hi))

        @pl.when(s == kv_at)
        def _():
            kv_total()

        @pl.when(s == end - hop_lag * TWO + ONE)
        def _():
            gain_total()

        return carry

    lax.fori_loop(ZERO, end + TWO, step, ZERO)
    far_waits(True)
    far_waits(False, first_b)
    kv_settle()


def back_call(att, act, wod, gate, up, dact, dq, wcat, wkv, dkv, table, h, dy, x, gain, nc=12, col=1024, tile=512):
    tok, width = h.shape
    inner, ff = att.shape[1], act.shape[1]
    ka, kb, kv = inner + ff, wcat.shape[1], dkv.shape[1]
    cr = tok // (2 * nc)
    rt_rows = 4 * cr
    blk, mid = width // 8, width // 2
    na, nb = ka // tile, (kb + kv) // tile
    big = max(mid, 2 * tile)
    shape = jax.ShapeDtypeStruct
    outs = (
        shape((tok, width), BF16), shape((tok, width), BF16), shape((2, tok, width), BF16), shape((2, 2 * nc, cr, width), BF16),
        shape((2, nc, cr, kv), BF16), shape((tok, kb + kv), BF16), shape((nc * cr, width), F32),
        shape((ka, mid), F32), shape((mid, kb + kv), F32), shape((ka, blk), F32), shape((blk, kb + kv), F32),
        shape((3, ka, blk), WIRE), shape((3, blk, kb + kv), WIRE), shape((2, 8, blk), F32), shape((8, 8, blk), F32), shape((2, blk, kv), F32),
        shape((3, ka, blk), WIRE), shape((3, blk, kb + kv), WIRE),
    )
    sems = pltpu.SemaphoreType.DMA
    scratch = [
        pltpu.VMEM((max(ka, tok), width), BF16), pltpu.VMEM((width, kb), BF16), pltpu.VMEM((2, tok, tile), BF16),
        pltpu.VMEM((width, kv), BF16), pltpu.VMEM(table.shape, F32),
        pltpu.VMEM((rt_rows, max(ka, kb)), BF16), pltpu.VMEM((rt_rows, max(ff, width)), BF16),
        pltpu.VMEM((big, big), F32), pltpu.VMEM((mid, tile), F32),
        pltpu.VMEM((2, 3, tile, blk), WIRE), pltpu.VMEM((2, 3, blk, tile), WIRE),
        pltpu.VMEM((2, cr, width), BF16), pltpu.VMEM((2, cr, width), BF16), pltpu.VMEM((2, 3, cr, width), BF16),
        pltpu.VMEM((cr, width), BF16), pltpu.VMEM((cr, width), BF16), pltpu.VMEM((cr, width), F32),
        pltpu.VMEM((2, cr, kv), BF16), pltpu.VMEM((2, cr, kv), BF16), pltpu.VMEM((2, 3, cr, kv), BF16),
        pltpu.VMEM((16, width), F32), pltpu.VMEM((blk, kv), F32), pltpu.VMEM((8, 8, blk), F32),
        sems((5,)), sems((11,)), sems, sems((2, 7)), sems((2, 3)), sems((2,)),
        sems((2, 2 * nc)), sems((2, 2 * nc)), sems((2, nc)), sems((2, nc)), sems((2, 2 * nc)), sems((2, 2 * nc)),
        sems((na + nb,)), sems((na + nb,)), sems((3, na + nb)), sems((3, na + nb)), sems((2 + mid // tile,)), sems((2, 3)),
        sems((3,)), sems((2,)), sems, sems((8,)), sems((8,)), sems((8,)), sems((3,)), sems((2,)),
    ]
    flops = 2 * tok * width * (2 * ka + 2 * kb)
    anywhere = pl.BlockSpec(memory_space=pl.ANY)
    return pl.pallas_call(
        functools.partial(back_kernel, (nc, cr, col, tile)),
        out_shape=outs,
        in_specs=[anywhere] * 15,
        out_specs=tuple(anywhere for _ in outs),
        scratch_shapes=scratch,
        cost_estimate=pl.CostEstimate(flops=2 * flops, bytes_accessed=200_000_000, transcendentals=tok * ff),
        compiler_params=pltpu.CompilerParams(vmem_limit_bytes=67_000_000, has_side_effects=True),
        name='backward',
    )(att, act, wod, gate, up, dact, dq, wcat, wkv, dkv, table, h, dy, x, gain)


def attention_kernel(heads, qkv, datt, table, att, dq, dkv, krot, dk_acc, dv_acc):
    n_pos = qkv.shape[0]
    head = qkv.shape[1] // (heads + 2)
    half = head // 2
    scale = 1.0 / math.sqrt(head)
    qb = 256

    def cos_of(sl):
        return table[sl, 0:half], table[sl, half:head]

    def turn(lo, sl, factor):
        cos_t, sin_t = cos_of(sl)
        first = qkv[sl, lo:lo + half].astype(F32)
        second = qkv[sl, lo + half:lo + head].astype(F32)
        return jnp.concatenate([(first * cos_t - second * sin_t) * factor, (second * cos_t + first * sin_t) * factor], axis=-1).astype(BF16)

    k_at, v_at = heads * head, (heads + 1) * head
    krot[...] = turn(k_at, slice(0, n_pos), 1.0)
    dk_acc[...] = jnp.zeros_like(dk_acc)
    dv_acc[...] = jnp.zeros_like(dv_acc)
    for r in range(heads):
        for i in range(n_pos // qb):
            sl = slice(i * qb, (i + 1) * qb)
            upto = (i + 1) * qb
            q = turn(r * head, sl, scale)
            k = krot[0:upto, :]
            v = qkv[0:upto, v_at:v_at + head]
            scores = contract(q, k, (1, 1))
            rows = lax.broadcasted_iota(jnp.int32, (qb, upto), 0) + i * qb
            scores = jnp.where(rows >= lax.broadcasted_iota(jnp.int32, (qb, upto), 1), scores, -1e30)
            exp_val = jnp.exp(scores - jnp.max(scores, axis=-1, keepdims=True))
            prob = exp_val / jnp.sum(exp_val, axis=-1, keepdims=True)
            prob_b = prob.astype(BF16)
            att[sl, r * head:(r + 1) * head] = contract(prob_b, v, (1, 0)).astype(BF16)
            do = datt[sl, r * head:(r + 1) * head]
            d_prob = contract(do, v, (1, 1)).astype(BF16).astype(F32)
            d_scores = (prob * (d_prob - jnp.sum(d_prob * prob, axis=-1, keepdims=True))).astype(BF16)
            d_rot = contract(d_scores, k, (1, 0)).astype(BF16).astype(F32) * scale
            cos_t, sin_t = cos_of(sl)
            first, second = d_rot[:, 0:half], d_rot[:, half:head]
            dq[sl, r * head:r * head + half] = (first * cos_t + second * sin_t).astype(BF16)
            dq[sl, r * head + half:(r + 1) * head] = (second * cos_t - first * sin_t).astype(BF16)
            dk_acc[0:upto, :] += contract(d_scores, q, (0, 0))
            dv_acc[0:upto, :] += contract(prob_b, do, (0, 0))
    dkv[:, 0:head] = dk_acc[...].astype(BF16)
    dkv[:, head:2 * head] = dv_acc[...].astype(BF16)


def attention_call(qkv, datt, table, n_batch):
    tok, wide = qkv.shape
    inner = datt.shape[1]
    head = table.shape[1]
    n_pos = tok // n_batch
    heads = inner // head

    def rows(n):
        return pl.BlockSpec((n_pos, n), lambda b: (b, 0))

    shape = jax.ShapeDtypeStruct
    flops = 2 * n_batch * heads * n_pos * n_pos * head * 7
    return pl.pallas_call(
        functools.partial(attention_kernel, heads),
        grid=(n_batch,),
        out_shape=(shape((tok, inner), BF16), shape((tok, inner), BF16), shape((tok, 2 * head), BF16)),
        in_specs=[rows(wide), rows(inner), pl.BlockSpec(table.shape, lambda b: (0, 0))],
        out_specs=(rows(inner), rows(inner), rows(2 * head)),
        scratch_shapes=[pltpu.VMEM((n_pos, head), BF16), pltpu.VMEM((n_pos, head), F32), pltpu.VMEM((n_pos, head), F32)],
        cost_estimate=pl.CostEstimate(flops=flops, bytes_accessed=20_000_000, transcendentals=n_batch * heads * n_pos * n_pos),
        compiler_params=pltpu.CompilerParams(vmem_limit_bytes=67_000_000),
        name='attention',
    )(qkv, datt, table)


def finish_kernel(y, gx, own_o, own_d, got_o, got_d, own_b, got_b, kvs, y_out, gx_out, o_out, d_out, g_out, u_out, q_out, k_out, v_out):
    y_out[...] = y[...]
    gx_out[...] = gx[...]

    def total(own, got):
        return own[...] + got[0].astype(F32) + got[1].astype(F32) + got[2].astype(F32)

    o_out[...] = total(own_o, got_o)
    d_out[...] = total(own_d, got_d)
    ff, inner, head = g_out.shape[1], q_out.shape[1], k_out.shape[1]
    at = 0
    for out in (g_out, u_out, q_out):
        cols = slice(at, at + out.shape[1])
        out[...] = own_b[:, cols] + got_b[0, :, cols].astype(F32) + got_b[1, :, cols].astype(F32) + got_b[2, :, cols].astype(F32)
        at += out.shape[1]
    k_out[...] = kvs[0, :, 0:head] + kvs[1, :, 0:head]
    v_out[...] = kvs[0, :, head:] + kvs[1, :, head:]


def finish_call(y, gx, own_a, got_a, own_b, got_b, kvs, inner, ff, steps=16):
    tok, width = y.shape
    blk, wide = own_b.shape
    kv = kvs.shape[2]
    skip = inner // (ff // steps)
    shape = jax.ShapeDtypeStruct

    def rows(n, cols, off=0):
        return pl.BlockSpec((n // steps, cols), lambda i: (i + off, 0))

    def three(n, cols, off=0):
        return pl.BlockSpec((3, n // steps, cols), lambda i: (0, i + off, 0))

    used = 2 * ff + inner
    return pl.pallas_call(
        finish_kernel,
        grid=(steps,),
        out_shape=(shape((tok, width), BF16), shape((tok, width), BF16), shape((inner, blk), F32), shape((ff, blk), F32),
                   shape((blk, ff), F32), shape((blk, ff), F32), shape((blk, inner), F32), shape((blk, kv // 2), F32), shape((blk, kv // 2), F32)),
        in_specs=[rows(tok, width), rows(tok, width), rows(inner, blk), rows(ff, blk, skip), three(inner, blk), three(ff, blk, skip),
                  rows(blk, used), three(blk, used), pl.BlockSpec((2, blk // steps, kv), lambda i: (0, i, 0))],
        out_specs=(rows(tok, width), rows(tok, width), rows(inner, blk), rows(ff, blk), rows(blk, ff), rows(blk, ff), rows(blk, inner),
                   rows(blk, kv // 2), rows(blk, kv // 2)),
        cost_estimate=pl.CostEstimate(flops=8 * blk * wide, bytes_accessed=66_000_000, transcendentals=0),
        compiler_params=pltpu.CompilerParams(vmem_limit_bytes=67_000_000),
        name='finish',
    )(y, gx, own_a, own_a, got_a, got_a, own_b, got_b, kvs)


def solution(mesh):
    def device_step(x_in, dy_out, ln_gain, w_q, w_k, w_v, w_o, w_gate, w_up, w_down):
        n_batch, seq_len, width = x_in.shape
        head_dim = w_k.shape[1]
        inner = w_q.shape[1]
        ff = w_gate.shape[1]
        tok = n_batch * seq_len
        x_rows = x_in.reshape(tok, width)
        dy = dy_out.reshape(tok, width)
        table = jnp.concatenate(rope_tables(seq_len, head_dim), axis=-1)

        gain8 = jnp.broadcast_to(ln_gain[None, :], (8, ln_gain.shape[0]))
        front = front_call(x_rows, dy, gain8, (w_q, w_k, w_v, w_o, w_down, w_gate, w_up))
        wcat, wkv, wod, gain, h_norm, qkv, gate, up, act, d_att, d_act = front
        att, d_q, dkv = attention_call(qkv, d_att, table, n_batch)
        res = back_call(att, act, wod, gate, up, d_act, d_q, wcat, wkv, dkv, table, h_norm, dy, x_rows, gain)
        own_a, own_b, got_a, got_b, gsum, _, kvsum = res[9:16]
        done = finish_call(res[0], res[1], own_a, got_a, own_b, got_b, kvsum, inner, ff)
        y_rows, gx_rows, grad_wo, grad_wdown, grad_wgate, grad_wup, grad_wq, grad_wk, grad_wv = done
        grad_gain = gsum[0, 0] + gsum[1, 0]
        return (y_rows.reshape(x_in.shape), gx_rows.reshape(x_in.shape), grad_gain, grad_wq, grad_wk, grad_wv,
                grad_wo, grad_wgate, grad_wup, grad_wdown)

    act_spec = P('fsdp', None, None)
    row_spec = P('fsdp', 'tp')
    kv_spec = P('fsdp', None)
    col_spec = P('tp', 'fsdp')
    in_specs = (act_spec, act_spec, P('fsdp'), row_spec, kv_spec, kv_spec, col_spec, row_spec, row_spec, col_spec)
    out_specs = (act_spec, act_spec, P('fsdp'), row_spec, kv_spec, kv_spec, col_spec, row_spec, row_spec, col_spec)
    return jax.shard_map(device_step, mesh=mesh, in_specs=in_specs, out_specs=out_specs, check_vma=False)
```

```python
import functools
import math
import jax
import jax.numpy as jnp
from jax import lax
from jax.experimental import pallas as pl
from jax.experimental.pallas import tpu as pltpu
from jax.sharding import PartitionSpec as P

F32 = jnp.float32
BF16 = jnp.bfloat16
WIRE = jnp.bfloat16
STEP = 32
ZERO, ONE, TWO, THREE = range(4)


def rope_tables(seq_len, head_dim):
    half_dim = head_dim // 2
    inv_freq = jnp.power(10000.0, -2.0 * jnp.arange(half_dim, dtype=F32) / head_dim)
    angle = jnp.arange(seq_len, dtype=F32)[:, None] * inv_freq[None, :]
    return jnp.cos(angle), jnp.sin(angle)


def row_loop(rows, fn):
    def body(i, carry):
        fn(pl.ds(pl.multiple_of(i * STEP, STEP), STEP))
        return carry

    lax.fori_loop(0, rows // STEP, body, 0)


def contract(left, right, dims):
    return lax.dot_general(left, right, ((dims[:1], dims[1:]), ((), ())), preferred_element_type=F32)


def front_kernel(dims, x, dy, gain, sq, sk, sv, so, sd, sg, su,
                 wcat, wkv, wod, gain_all, h, qkv, gate, up, act, datt, dact,
                 hv, wv, wodv, wqv, xt, yt, gt, et, b_q, b_k, b_v, b_o, b_d, b_g, b_u, gv,
                 load, wload, keep, bsem, gsem, gain_s, gain_r, send, recv):
    rt_rows, split = dims
    tok, width = x.shape
    inner, head, ff = sq.shape[ONE], sk.shape[ONE], sg.shape[ONE]
    kv = TWO * head
    blk = sq.shape[ZERO]
    ka = inner + ff
    n = tok // rt_rows
    me = lax.axis_index('fsdp')

    def local(src, dst, sem):
        return pltpu.make_async_copy(src, dst, sem)

    def remote(src, dst, s, r, to):
        return pltpu.make_async_remote_copy(src_ref=src, dst_ref=dst, send_sem=s, recv_sem=r, device_id={'fsdp': me ^ to},
                                            device_id_type=pl.DeviceIdType.MESH)

    items = (
        (sq, wcat, TWO * ff, inner, False), (sk, wkv, ZERO, head, False), (sv, wkv, head, head, False),
        (so, wod, ZERO, inner, True), (sd, wod, inner, ff, True), (sg, wcat, ZERO, ff, False), (su, wcat, ff, ff, False),
    )
    group_q, group_o, group_g, group_u = (ZERO, ONE, TWO), (THREE, 4), (5,), (6,)

    def block(i, mask, part=None):
        _, whole_w, at, wide, tall = items[i]
        at_blk = pl.multiple_of((me ^ mask) * blk, blk)
        if tall:
            rows = pl.ds(at, wide) if part is None else pl.ds(at + part * (wide // TWO), wide // TWO)
            return whole_w.at[rows, pl.ds(at_blk, blk)]
        rows = pl.ds(at_blk, blk) if part is None else pl.ds(at_blk + part * (blk // TWO), blk // TWO)
        return whole_w.at[rows, pl.ds(at, wide)]

    def own_to(i, to, num):
        return remote(items[i][ZERO], block(i, ZERO), send.at[i, num], recv.at[i, num], to)

    def pass_to(i, mask, to, num, part=None):
        return remote(block(i, mask, part), block(i, mask, part), send.at[i, num], recv.at[i, num], to)

    def arrived(i, mask, to, num, part=None):
        remote(block(i, mask, part), block(i, mask, part), send.at[i, num], recv.at[i, num], to).wait_recv()

    def depart(group):
        for i in group:
            own_to(i, TWO, ZERO).start()
            own_to(i, 4, ONE).start()
            own_to(i, ONE, 4).start()

    def relay(group):
        for i in group:
            arrived(i, TWO, TWO, ZERO)
            pass_to(i, TWO, 4, TWO, ZERO).start()
            arrived(i, 4, 4, ONE)
            pass_to(i, 4, TWO, THREE, ONE).start()
            pass_to(i, TWO, ONE, 5).start()
            pass_to(i, 4, ONE, 6).start()

    def corner(group):
        for i in group:
            arrived(i, 6, 4, TWO, ZERO)
            pass_to(i, 6, ONE, 7, ZERO).start()
            arrived(i, 6, TWO, THREE, ONE)
            pass_to(i, 6, ONE, 8, ONE).start()

    def full(group):
        for i in group:
            arrived(i, ONE, ONE, 4)
            arrived(i, THREE, ONE, 5)
            arrived(i, 5, ONE, 6)
            arrived(i, 7, ONE, 7, ZERO)
            arrived(i, 7, ONE, 8, ONE)

    def sent(i):
        own_to(i, TWO, ZERO).wait_send()
        own_to(i, 4, ONE).wait_send()
        own_to(i, ONE, 4).wait_send()
        pass_to(i, TWO, 4, TWO, ZERO).wait_send()
        pass_to(i, 4, TWO, THREE, ONE).wait_send()
        pass_to(i, TWO, ONE, 5).wait_send()
        pass_to(i, 4, ONE, 6).wait_send()
        pass_to(i, 6, ONE, 7, ZERO).wait_send()
        pass_to(i, 6, ONE, 8, ONE).wait_send()

    bounce = (b_q, b_k, b_v, b_o, b_d, b_g, b_u)

    def own_in(i):
        return local(items[i][ZERO], bounce[i], bsem.at[i])

    def own_out(i):
        return local(bounce[i], block(i, ZERO), bsem.at[i])

    def tile_rows(k):
        return pl.ds(pl.multiple_of(k * rt_rows, rt_rows), rt_rows)

    def tiles(fn):
        def body(k, carry):
            fn(k)
            return carry

        lax.fori_loop(ZERO, n, body, ZERO)

    def dot_cols(left, weight, dims_, out, wide):
        col = wide // split

        def body(j, carry):
            cs = pl.ds(pl.multiple_of(j * col, col), col)
            rhs = weight[:, cs] if dims_[ONE] == ZERO else weight[cs, :]
            out[:, cs] = contract(left[...], rhs, dims_).astype(BF16)
            return carry

        lax.fori_loop(ZERO, split, body, ZERO)

    def gain_cols(mask):
        return pl.ds(pl.multiple_of((me ^ mask) * blk, blk), blk)

    def gain_to(m):
        return remote(gain, gain_all.at[:, gain_cols(ZERO)], gain_s.at[m - ONE], gain_r.at[m - ONE], m)

    def gain_from(m):
        return remote(gain, gain_all.at[:, gain_cols(m)], gain_s.at[m - ONE], gain_r.at[m - ONE], m)

    def gain_in(m):
        return local(gain if m == ZERO else gain_all.at[:, gain_cols(m)], gv.at[:, gain_cols(m)], gsem.at[m])

    peers = range(ONE, 8)
    for m in peers:
        gain_to(m).start()
    depart(group_q)
    gain_in(ZERO).start()
    n_items = len(items)
    for i in range(n_items):
        own_in(i).start()
    for m in peers:
        gain_from(m).wait_recv()
        gain_in(m).start()
    for i in range(n_items):
        own_in(i).wait()
        own_out(i).start()
    for m in range(8):
        gain_in(m).wait()

    def x_load(k):
        return local(x.at[tile_rows(k)], xt.at[lax.rem(k, TWO)], load.at[lax.rem(k, TWO)])

    def h_keep(k):
        return local(hv.at[tile_rows(k)], h.at[tile_rows(k)], keep.at[lax.rem(k, TWO)])

    x_load(ZERO).start()

    def norm(k):
        x_load(k).wait()

        @pl.when(k + ONE < n)
        def _():
            x_load(k + ONE).start()

        def rows(sl):
            xv = xt[lax.rem(k, TWO), sl, :].astype(F32)
            cent = xv - jnp.mean(xv, axis=-ONE, keepdims=True)
            inv = lax.rsqrt(jnp.mean(cent * cent, axis=-ONE, keepdims=True) + 1e-5)
            hv[pl.ds(pl.multiple_of(k * rt_rows + sl.start, STEP), STEP), :] = (cent * inv * gv[ZERO:ONE, :]).astype(BF16)

        row_loop(rt_rows, rows)

        @pl.when(k >= TWO)
        def _():
            h_keep(k - TWO).wait()

        h_keep(k).start()

        @pl.when(k == n // TWO)
        def _():
            relay(group_q)
            depart(group_o)

    tiles(norm)
    h_keep(n - TWO).wait()
    h_keep(n - ONE).wait()

    corner(group_q)
    for i in range(n_items):
        own_out(i).wait()
    full(group_q)
    w0 = local(wcat.at[:, pl.ds(TWO * ff, inner)], wqv.at[:, pl.ds(ZERO, inner)], wload.at[ZERO])
    w1 = local(wkv, wqv.at[:, pl.ds(inner, kv)], wload.at[ONE])
    w0.start()
    w1.start()
    w0.wait()
    w1.wait()

    def after_store(k, copies):
        @pl.when(k >= TWO)
        def _():
            for c in copies(k - TWO):
                c.wait()

    def stored(copies):
        for k in range(max(n - TWO, ZERO), n):
            for c in copies(k):
                c.wait()

    def half(ref, k, at, wide):
        return ref.at[lax.rem(k, TWO), :, pl.ds(at, wide)]

    def qkv_keep(k):
        return (local(half(yt, k, ZERO, inner + kv), qkv.at[tile_rows(k)], keep.at[lax.rem(k, TWO)]),)

    def qkv_tile(k):
        after_store(k, qkv_keep)
        dot_cols(hv.at[tile_rows(k)], wqv, (ONE, ZERO), yt.at[lax.rem(k, TWO)], inner + kv)
        for c in qkv_keep(k):
            c.start()

    tiles(qkv_tile)
    stored(qkv_keep)

    def dy_load(k):
        return local(dy.at[tile_rows(k)], xt.at[lax.rem(k, TWO)], load.at[lax.rem(k, TWO)])

    dy_load(ZERO).start()
    relay(group_o)
    depart(group_g)
    corner(group_o)
    full(group_o)
    w2 = local(wod, wodv, wload.at[TWO])
    w2.start()
    w2.wait()

    def back_keep(k):
        return (local(half(yt, k, ZERO, inner), datt.at[tile_rows(k)], keep.at[lax.rem(k, TWO)]),
                local(half(yt, k, inner, ff), dact.at[tile_rows(k)], keep.at[TWO + lax.rem(k, TWO)]))

    def back_tile(k):
        dy_load(k).wait()

        @pl.when(k + ONE < n)
        def _():
            dy_load(k + ONE).start()

        after_store(k, back_keep)
        dot_cols(xt.at[lax.rem(k, TWO)], wodv, (ONE, ONE), yt.at[lax.rem(k, TWO)], ka)
        for c in back_keep(k):
            c.start()

        @pl.when(k == n // TWO)
        def _():
            relay(group_g)
            depart(group_u)

    tiles(back_tile)
    stored(back_keep)

    corner(group_g)
    full(group_g)
    w3 = local(wcat.at[:, pl.ds(ZERO, ff)], wv, wload.at[THREE])
    w3.start()
    w3.wait()

    def gate_keep(k):
        return (local(half(yt, k, ZERO, ff), gate.at[tile_rows(k)], keep.at[lax.rem(k, TWO)]),)

    def gate_tile(k):
        after_store(k, gate_keep)
        dot_cols(hv.at[tile_rows(k)], wv, (ONE, ZERO), yt.at[lax.rem(k, TWO)], ff)
        for c in gate_keep(k):
            c.start()

        @pl.when(k == n // TWO)
        def _():
            relay(group_u)

    tiles(gate_tile)
    stored(gate_keep)

    def gate_load(k):
        return local(gate.at[tile_rows(k)], gt, load.at[TWO])

    gate_load(ZERO).start()
    corner(group_u)
    full(group_u)
    w4 = local(wcat.at[:, pl.ds(ff, ff)], wv, wload.at[4])
    w4.start()
    w4.wait()

    def up_keep(k):
        return (local(half(yt, k, ZERO, ff), up.at[tile_rows(k)], keep.at[lax.rem(k, TWO)]),
                local(et.at[lax.rem(k, TWO)], act.at[tile_rows(k)], keep.at[TWO + lax.rem(k, TWO)]))

    def up_tile(k):
        after_store(k, up_keep)
        dot_cols(hv.at[tile_rows(k)], wv, (ONE, ZERO), yt.at[lax.rem(k, TWO)], ff)
        gate_load(k).wait()

        def rows(sl):
            g = gt[sl, :].astype(F32)
            et[lax.rem(k, TWO), sl, :] = (g * jax.nn.sigmoid(g) * yt[lax.rem(k, TWO), sl, ZERO:ff].astype(F32)).astype(BF16)

        row_loop(rt_rows, rows)

        @pl.when(k + ONE < n)
        def _():
            gate_load(k + ONE).start()

        for c in up_keep(k):
            c.start()

    tiles(up_tile)
    stored(up_keep)
    for i in range(n_items):
        sent(i)
    for m in peers:
        gain_to(m).wait_send()
    g_out = local(gv.at[:, gain_cols(ZERO)], gain_all.at[:, gain_cols(ZERO)], gsem.at[ZERO])
    g_out.start()
    g_out.wait()


def front_call(x, dy, gain, shards, rt_rows=384, split=2):
    sq, sk, sv, so, sd, sg, su = shards
    tok, width = x.shape
    inner, ff = sq.shape[1], sg.shape[1]
    kv = 2 * sk.shape[1]
    ka = inner + ff
    blk = sq.shape[0]
    shape = jax.ShapeDtypeStruct
    outs = (
        shape((width, 2 * ff + inner), BF16), shape((width, kv), BF16), shape((ka, width), BF16), shape((8, width), F32),
        shape((tok, width), BF16), shape((tok, inner + kv), BF16), shape((tok, ff), BF16), shape((tok, ff), BF16), shape((tok, ff), BF16),
        shape((tok, inner), BF16), shape((tok, ff), BF16),
    )
    sems = pltpu.SemaphoreType.DMA
    scratch = [
        pltpu.VMEM((tok, width), BF16), pltpu.VMEM((width, ff), BF16), pltpu.VMEM((ka, width), BF16), pltpu.VMEM((width, inner + kv), BF16),
        pltpu.VMEM((2, rt_rows, width), BF16), pltpu.VMEM((2, rt_rows, max(ka, inner + kv)), BF16), pltpu.VMEM((rt_rows, ff), BF16),
        pltpu.VMEM((2, rt_rows, ff), BF16), *[pltpu.VMEM(w.shape, BF16) for w in shards],
        pltpu.VMEM((8, width), F32),
        sems((3,)), sems((5,)), sems((4,)), sems((7,)), sems((8,)), sems((7,)), sems((7,)), sems((7, 9)), sems((7, 9)),
    ]
    flops = 2 * tok * width * (2 * ka + ff + kv)
    anywhere = pl.BlockSpec(memory_space=pl.ANY)
    return pl.pallas_call(
        functools.partial(front_kernel, (rt_rows, split)),
        out_shape=outs,
        in_specs=[anywhere] * 10,
        out_specs=tuple(anywhere for _ in outs),
        scratch_shapes=scratch,
        cost_estimate=pl.CostEstimate(flops=flops, bytes_accessed=150_000_000, transcendentals=tok * ff),
        compiler_params=pltpu.CompilerParams(vmem_limit_bytes=67_000_000, has_side_effects=True),
        name='forward',
    )(x, dy, gain, *shards)


def back_kernel(dims, att, act, wod, gate, up, dact, dq, wcat, wkv, dkv, table, h, dy, x, gain,
                y_out, gx_out, part, line, kvline, dcat, dhkv, peer_a, peer_b, own_a, own_b, got_a, got_b, gsum, gtmp, kvsum, snd_a, snd_b,
                wa, wb, st, wv, tv, ctile, gt, ot, rt, sa, sb, zr, zo, zs, zx, zd, zk, kr, ko, kz, gv, kw, gw,
                load, wload, wait_y, zload, zstore, kstore, rs_s, rs_r, kv_s, kv_r, ag_s, ag_r, core_s, core_r, far_s, far_r, own_s, put_s, kf_s, kf_r, kf_l, gl_s, gf_s, gf_r, gz_s, gz_r):
    nc, cr, col, tile = dims
    tok, width = h.shape
    inner, ff = att.shape[ONE], act.shape[ONE]
    ka, kb = inner + ff, wcat.shape[ONE]
    kv = dkv.shape[ONE]
    head = kv // TWO
    n_pos = table.shape[ZERO]
    rt_rows = 4 * cr
    blk = width // 8
    mid = width // TWO
    na, nb = ka // tile, (kb + kv) // tile
    depth = THREE
    last = THREE
    hop_lag, pass_lag = ONE, ONE
    end = TWO * nc - ONE + hop_lag * last + pass_lag * TWO
    me = lax.axis_index('fsdp')
    z = lax.axis_index('tp')

    def remote(src, dst, send, recv, **to):
        return pltpu.make_async_remote_copy(src_ref=src, dst_ref=dst, send_sem=send, recv_sem=recv,
                                            device_id=to, device_id_type=pl.DeviceIdType.MESH)

    def local(src, dst, sem):
        return pltpu.make_async_copy(src, dst, sem)

    def chunk_row(d, c):
        return pl.multiple_of(lax.rem(c, nc) * (TWO * cr) + d * cr, cr)

    def chunk_rows(d, c):
        return pl.ds(chunk_row(d, c), cr)

    def slot_parts(t):
        parts = []
        up_z, down_z = lax.rem(z + ONE, last + ONE), lax.rem(z + last, last + ONE)
        for d in range(TWO):
            parts.append(line_parts(t, d, up_z, down_z))
        return parts

    def line_parts(t, d, up_z, down_z):
        if True:
            rank = z if d == ZERO else last - z
            fwd, back = (up_z, down_z) if d == ZERO else (down_z, up_z)

            def hop(c, src=None):
                src = part.at[lax.div(c, nc), chunk_rows(d, c)] if src is None else src
                return remote(src, line.at[d, c], rs_s.at[d, c], rs_r.at[d, c], tp=fwd)

            def mid_hop(c):
                return hop(c, zs.at[d, lax.rem(c, depth)])

            def kv_hop(c, src=None):
                src = dkv.at[chunk_rows(d, c)] if src is None else src
                return remote(src, kvline.at[d, c], kv_s.at[d, c], kv_r.at[d, c], tp=fwd)

            def mid_kv_hop(c):
                return kv_hop(c, kz.at[d, lax.rem(c, depth)])

            def bcast_of(c, dst, src=None):
                src = dst.at[chunk_rows(d, c)] if src is None else src
                return remote(src, dst.at[chunk_rows(d, c)], ag_s.at[d, c], ag_r.at[d, c], tp=back)

            def keep_of(c, dst):
                return local(zs.at[d, lax.rem(c, depth)], dst.at[chunk_rows(d, c)], zstore.at[d, lax.rem(c, depth)])

            def for_kind(c, fn):
                @pl.when(c < nc)
                def _():
                    fn(y_out)

                @pl.when(c >= nc)
                def _():
                    fn(gx_out)

            def depart():
                @pl.when((rank == ZERO) & (t >= ZERO) & (t < TWO * nc))
                def _():
                    hop(t).start()

                    @pl.when(t < nc)
                    def _():
                        kv_hop(t).start()

            c = t - hop_lag * rank
            rows = chunk_rows(d, c)
            own = pl.ds(pl.multiple_of(lax.rem(c, nc) * cr, cr), cr)

            def load_of(i):
                return (
                    local(part.at[lax.div(c, nc), rows], zo.at[d], zload.at[d, ZERO]), local(line.at[d, c], zr.at[d], zload.at[d, ONE]),
                    local(x.at[rows], zx, zload.at[d, TWO]), local(dy.at[rows], zd, zload.at[d, THREE]),
                    local(dhkv.at[own], zk, zload.at[d, 4]), local(dkv.at[rows], ko.at[d], zload.at[d, 5]),
                    local(kvline.at[d, lax.rem(c, nc)], kr.at[d], zload.at[d, 6]),
                )[i]

            busy = (rank > ZERO) & (c >= ZERO) & (c < TWO * nc)

            def begin():
                @pl.when(busy)
                def _():
                    load_of(ZERO).start()

                    @pl.when(rank == last)
                    def _():
                        load_of(TWO).start()

                        @pl.when(c >= nc)
                        def _():
                            load_of(THREE).start()

                    hop(c).wait_recv()
                    load_of(ONE).start()

                    @pl.when(c < nc)
                    def _():
                        load_of(5).start()
                        kv_hop(c).wait_recv()
                        load_of(6).start()

            def finish():
                @pl.when(busy & (rank < last))
                def _():
                    @pl.when(c >= depth)
                    def _():
                        mid_hop(c - depth).wait_send()

                    load_of(ZERO).wait()
                    load_of(ONE).wait()

                    def add(sl):
                        zs[d, lax.rem(c, depth), sl, :] = (zr[d, sl, :].astype(F32) + zo[d, sl, :].astype(F32)).astype(BF16)

                    row_loop(cr, add)
                    mid_hop(c).start()

                    @pl.when(c < nc)
                    def _():
                        @pl.when(c >= depth)
                        def _():
                            mid_kv_hop(c - depth).wait_send()

                        load_of(5).wait()
                        load_of(6).wait()
                        kz[d, lax.rem(c, depth)] = (kr[d].astype(F32) + ko[d].astype(F32)).astype(BF16)
                        mid_kv_hop(c).start()

                @pl.when(busy & (rank == last))
                def _():
                    @pl.when(c >= nc)
                    def _():
                        load_of(4).start()

                    @pl.when(c >= depth)
                    def _():
                        bcast_of(c - depth, y_out).wait_send()
                        keep_of(c - depth, y_out).wait()

                    load_of(ZERO).wait()
                    load_of(ONE).wait()
                    load_of(TWO).wait()

                    @pl.when(c < nc)
                    def _():
                        def fin(sl):
                            branch = zr[d, sl, :].astype(F32) + zo[d, sl, :].astype(F32)
                            zs[d, lax.rem(c, depth), sl, :] = (zx[sl, :].astype(F32) + branch).astype(BF16)

                        row_loop(cr, fin)

                    @pl.when(c >= nc)
                    def _():
                        load_of(THREE).wait()
                        load_of(4).wait()

                        def fin(sl):
                            dh = (zr[d, sl, :].astype(F32) + zo[d, sl, :].astype(F32) + zk[sl, :]).astype(BF16).astype(F32)
                            xv = zx[sl, :].astype(F32)
                            cent = xv - jnp.mean(xv, axis=-ONE, keepdims=True)
                            inv = lax.rsqrt(jnp.mean(cent * cent, axis=-ONE, keepdims=True) + 1e-5)
                            hat = cent * inv
                            gv[8:9, :] = gv[8:9, :] + jnp.sum(dh * hat, axis=ZERO, keepdims=True)
                            dn = dh * gv[ZERO:ONE, :]
                            dx = inv * (dn - jnp.mean(dn, axis=-ONE, keepdims=True)
                                        - hat * jnp.mean(dn * hat, axis=-ONE, keepdims=True))
                            zs[d, lax.rem(c, depth), sl, :] = (zd[sl, :].astype(F32) + dx).astype(BF16)

                        row_loop(cr, fin)

                    for_kind(c, lambda dst: keep_of(c, dst).start())
                    for_kind(c, lambda dst: bcast_of(c, dst, zs.at[d, lax.rem(c, depth)]).start())

                    @pl.when(c < nc)
                    def _():
                        load_of(5).wait()
                        load_of(6).wait()
                        pos = pl.ds(pl.multiple_of(lax.rem(chunk_row(d, c), n_pos), cr), cr)
                        cos_t, sin_t = tv[pos, ZERO:head // TWO], tv[pos, head // TWO:head]

                        def summed(lo, hi):
                            return (kr[d, :, lo:hi].astype(F32) + ko[d, :, lo:hi].astype(F32)).astype(BF16)

                        first = summed(ZERO, head // TWO).astype(F32)
                        second = summed(head // TWO, head).astype(F32)
                        kz[d, ZERO, :, ZERO:head // TWO] = (first * cos_t + second * sin_t).astype(BF16)
                        kz[d, ZERO, :, head // TWO:head] = (second * cos_t - first * sin_t).astype(BF16)
                        kz[d, ZERO, :, head:kv] = summed(head, kv)
                        keep_kv = local(kz.at[d, ZERO], dcat.at[rows, pl.ds(kb, kv)], kstore.at[ZERO])
                        keep_kv.start()

                        def cols(j, carry):
                            cs = pl.ds(pl.multiple_of(j * col, col), col)
                            zk[:, cs] = contract(kz[d, ZERO], wv[cs, :], (ONE, ONE))
                            return carry

                        lax.fori_loop(ZERO, width // col, cols, ZERO)
                        keep_h = local(zk, dhkv.at[own], kstore.at[ONE])
                        keep_h.start()
                        keep_kv.wait()
                        keep_h.wait()

            e = t - hop_lag * last - pass_lag * (last - rank)

            def pass_on():
                @pl.when(((rank == ONE) | (rank == TWO)) & (e >= ZERO) & (e < TWO * nc))
                def _():
                    bcast_of(e, y_out).wait_recv()
                    for_kind(e, lambda dst: bcast_of(e, dst).start())

            def settle():
                def each(c, carry):
                    tail = TWO * nc - depth
                    kv_tail = (c >= nc - depth) & (c < nc)

                    @pl.when(rank == ZERO)
                    def _():
                        hop(c).wait_send()
                        bcast_of(c, y_out).wait_recv()

                        @pl.when(c < nc)
                        def _():
                            kv_hop(c).wait_send()

                    @pl.when((rank == ONE) | (rank == TWO))
                    def _():
                        bcast_of(c, y_out).wait_send()

                        @pl.when(c >= tail)
                        def _():
                            mid_hop(c).wait_send()

                        @pl.when(kv_tail)
                        def _():
                            mid_kv_hop(c).wait_send()

                    @pl.when((rank == last) & (c >= tail))
                    def _():
                        bcast_of(c, y_out).wait_send()
                        keep_of(c, y_out).wait()

                    return carry

                lax.fori_loop(ZERO, TWO * nc, each, ZERO)

            return depart, begin, finish, pass_on, settle

    def slot(t):
        parts = slot_parts(t)
        for i in range(4):
            for p in parts:
                p[i]()

        @pl.when(t == end)
        def _():
            for p in parts:
                p[4]()

    def gain_total():
        low = pl.ds(8, 8)
        which = lax.div(z, last)

        def cols(mask):
            return pl.ds(pl.multiple_of((me ^ mask) * blk, blk), blk)

        def plane(m):
            return remote(gv.at[low, cols(m)], gtmp.at[m], gf_s.at[m], gf_r.at[m], fsdp=me ^ m)

        def along(i):
            return remote(gw.at[ZERO], gsum.at[which], gz_s.at[i], gz_r.at[which], tp=lax.rem(z + ONE + i, last + ONE))

        def arrived(w):
            remote(gw.at[ZERO], gsum.at[w], gz_s.at[ZERO], gz_r.at[w], tp=lax.rem(z + ONE, last + ONE)).wait_recv()

        peers = range(ONE, 8)

        @pl.when((z == ZERO) | (z == last))
        def _():
            for m in peers:
                plane(m).start()
            own = local(gv.at[low, cols(ZERO)], gw.at[ZERO], gl_s.at[ZERO])
            own.start()
            for m in peers:
                plane(m).wait_recv()
                local(gtmp.at[m], gw.at[m], gl_s.at[m]).start()
            own.wait()
            for m in peers:
                local(gtmp.at[m], gw.at[m], gl_s.at[m]).wait()
            gw[ZERO] = jnp.sum(gw[...], axis=ZERO)
            home = local(gw.at[ZERO], gsum.at[which], gl_s.at[ZERO])
            home.start()
            for i in range(THREE):
                along(i).start()
            home.wait()
            for m in peers:
                plane(m).wait_send()

        @pl.when(z != ZERO)
        def _():
            arrived(ZERO)

        @pl.when(z != last)
        def _():
            arrived(ONE)

        @pl.when((z == ZERO) | (z == last))
        def _():
            for i in range(THREE):
                along(i).wait_send()

    def tile_rows(k):
        return pl.ds(pl.multiple_of(k * rt_rows, rt_rows), rt_rows)

    def y_step(k):
        srcs = [local(att.at[tile_rows(k)], ctile.at[:, pl.ds(ZERO, inner)], load.at[ZERO]),
                local(act.at[tile_rows(k)], ctile.at[:, pl.ds(inner, ff)], load.at[ONE])]
        for s in srcs:
            s.start()
        for s in srcs:
            s.wait()

        def cols(j, carry):
            cs = pl.ds(pl.multiple_of(j * col, col), col)
            gt[:, cs] = contract(ctile[:, ZERO:ka], wa[ZERO:ka, cs], (ONE, ZERO)).astype(BF16)
            return carry

        lax.fori_loop(ZERO, width // col, cols, ZERO)
        dst = local(gt.at[:, pl.ds(ZERO, width)], part.at[ZERO, tile_rows(k)], wait_y)
        dst.start()
        dst.wait()

    def h_step(k):
        rows = tile_rows(k)
        srcs = [local(gate.at[rows], gt.at[:, pl.ds(ZERO, ff)], load.at[ZERO]), local(up.at[rows], ctile.at[:, pl.ds(ZERO, ff)], load.at[ONE]),
                local(dact.at[rows], ctile.at[:, pl.ds(ff, ff)], load.at[TWO]), local(dq.at[rows], ctile.at[:, pl.ds(TWO * ff, kb - TWO * ff)], load.at[THREE])]
        for s in srcs:
            s.start()
        for s in srcs:
            s.wait()

        def act_back(sl):
            g = gt[sl, ZERO:ff].astype(F32)
            u = ctile[sl, ZERO:ff].astype(F32)
            d_act = ctile[sl, ff:TWO * ff].astype(F32)
            sig = jax.nn.sigmoid(g)
            ctile[sl, ZERO:ff] = (d_act * u * (sig + g * sig * (1.0 - sig))).astype(BF16)
            ctile[sl, ff:TWO * ff] = (d_act * (g * sig)).astype(BF16)

        row_loop(rt_rows, act_back)
        keep = local(ctile, dcat.at[rows, pl.ds(ZERO, kb)], load.at[4])
        keep.start()

        def cols(j, carry):
            cs = pl.ds(pl.multiple_of(j * col, col), col)
            gt[:, cs] = contract(ctile[...], wb[cs, ZERO:kb], (ONE, ONE)).astype(BF16)
            return carry

        lax.fori_loop(ZERO, width // col, cols, ZERO)
        dst = local(gt.at[:, pl.ds(ZERO, width)], part.at[ONE, rows], wait_y)
        dst.start()
        dst.wait()
        keep.wait()

    def out_weights():
        return local(wod, wa.at[pl.ds(ZERO, ka)], wload.at[ZERO])

    def in_weights():
        return local(wcat, wb.at[pl.ds(ZERO, width), pl.ds(ZERO, kb)], wload.at[10])

    def operand(src):
        cps = []
        for q in range(8):
            mask = TWO * (q % 4) + q // 4
            cols = pl.ds(pl.multiple_of((me ^ mask) * blk, blk), blk)
            cps.append(local(src.at[:, cols], wa.at[pl.ds(ZERO, tok), pl.ds(q * blk, blk)], wload.at[q]))
        for c in cps:
            c.start()
        for c in cps:
            c.wait()

    first_b = -(-nb // TWO)

    def strip(is_a, k):
        if is_a:
            return k
        return jnp.where(k < first_b, k, jnp.where(k == first_b, nb - ONE, k - ONE))

    def wide_start(is_a, k):
        dst = st.at[lax.rem(k, TWO)]
        sem = wload.at[8 + lax.rem(k, TWO)]
        if is_a:
            @pl.when(k == ZERO)
            def _():
                local(att, dst, sem).start()

            @pl.when(k > ZERO)
            def _():
                local(act.at[:, pl.ds(pl.multiple_of((k - ONE) * tile, tile), tile)], dst, sem).start()
        else:
            local(dcat.at[:, pl.ds(pl.multiple_of(strip(is_a, k) * tile, tile), tile)], dst, sem).start()

    def wide(is_a, k, hi):
        local(dcat.at[:, pl.ds(ZERO, tile)], st.at[lax.rem(k, TWO)], wload.at[8 + lax.rem(k, TWO)]).wait()

        @pl.when(k + ONE < hi)
        def _():
            wide_start(is_a, k + ONE)

    def prod(is_a, k, odd):
        half = pl.ds(odd * mid, mid)
        if is_a:
            return contract(st[lax.rem(k, TWO)], wa[ZERO:tok, half], (ZERO, ZERO))
        return contract(wa[ZERO:tok, half], st[lax.rem(k, TWO)], (ZERO, ZERO))

    def place(ref, is_a, k):
        par = pl.multiple_of(lax.rem(k, TWO) * tile, tile)
        return ref.at[pl.ds(par, tile), :] if is_a else ref.at[:, pl.ds(par, tile)]

    def whole(ref, is_a, k):
        cs = pl.ds(pl.multiple_of(strip(is_a, k) * tile, tile), tile)
        return ref.at[cs, :] if is_a else ref.at[:, cs]

    def piece(ref, is_a, q):
        return ref.at[:, pl.ds(q * blk, blk)] if is_a else ref.at[pl.ds(q * blk, blk), :]

    def away(is_a, k, q):
        base, snd, got = (ZERO, snd_a, got_a) if is_a else (na, snd_b, got_b)
        return remote(whole(snd.at[q], is_a, k), whole(got.at[q], is_a, k), far_s.at[q, base + k], far_r.at[q, base + k],
                      fsdp=me ^ (TWO * (q + ONE)))

    def odd_steps(is_a, lo, hi, stop):
        base = ZERO if is_a else na
        peer = peer_a if is_a else peer_b

        def send(k):
            return remote(place(ot, is_a, k), whole(peer, is_a, k), core_s.at[base + k], core_r.at[base + k], fsdp=me ^ ONE)

        def one(k, carry):
            wide(is_a, k, hi)

            @pl.when(k >= stop[ZERO] + TWO)
            def _():
                send(k - TWO).wait_send()

            place(ot, is_a, k)[...] = prod(is_a, k, ONE)
            send(k).start()

            @pl.when(k == stop[ONE] - ONE)
            def _():
                send(k - ONE).wait_send()
                send(k).wait_send()

            return carry

        wide_start(is_a, lo)
        lax.fori_loop(lo, hi, one, ZERO)

    def even_steps(is_a, lo, hi, stop):
        base = ZERO if is_a else na
        peer, own, snd = (peer_a, own_a, snd_a) if is_a else (peer_b, own_b, snd_b)
        stage = sa if is_a else sb

        def take(k):
            return remote(place(ot, is_a, k), whole(peer, is_a, k), core_s.at[base + k], core_r.at[base + k], fsdp=me ^ ONE)

        def fetch(k):
            if not is_a:
                return [local(whole(peer, is_a, k), rt, own_s.at[TWO])]
            rows = pl.ds(pl.multiple_of(k * tile, tile), tile)
            return [local(peer.at[rows, pl.ds(i * tile, tile)], rt.at[pl.ds(i * tile, tile)], own_s.at[TWO + i])
                    for i in range(mid // tile)]

        def fetched():
            if not is_a:
                return rt[...]
            return jnp.concatenate([rt[i * tile:(i + ONE) * tile, :] for i in range(mid // tile)], axis=ONE)

        def mine(k):
            return local(piece(place(ot, is_a, k), is_a, ZERO), whole(own, is_a, k), own_s.at[lax.rem(k, TWO)])

        def put(k, q):
            return local(stage.at[lax.rem(k, TWO), q], whole(snd.at[q], is_a, k), put_s.at[lax.rem(k, TWO), q])

        def ship(k):
            for q in range(THREE):
                put(k, q).wait()
                away(is_a, k, q).start()

        def one(k, carry):
            take(k).wait_recv()
            for f in fetch(k):
                f.start()
            wide(is_a, k, hi)

            @pl.when(k >= stop[ZERO] + TWO)
            def _():
                mine(k - TWO).wait()

            acc = prod(is_a, k, ZERO)

            @pl.when(k >= stop[ZERO] + ONE)
            def _():
                ship(k - ONE)

            for f in fetch(k):
                f.wait()
            place(ot, is_a, k)[...] = acc + fetched()
            mine(k).start()
            for q in range(THREE):
                stage[lax.rem(k, TWO), q] = piece(place(ot, is_a, k), is_a, q + ONE)[...].astype(WIRE)
                put(k, q).start()

            @pl.when(k == stop[ONE] - ONE)
            def _():
                ship(k)
                mine(k - ONE).wait()
                mine(k).wait()

            return carry

        wide_start(is_a, lo)
        lax.fori_loop(lo, hi, one, ZERO)

    def far_wait(is_a, k):
        for q in range(THREE):
            away(is_a, k, q).wait_recv()

    def far_waits(is_a, but=-ONE):
        def one(k, carry):
            for q in range(THREE):
                away(is_a, k, q).wait_send()

            @pl.when(k != but)
            def _():
                far_wait(is_a, k)

            return carry

        lax.fori_loop(ZERO, na if is_a else nb, one, ZERO)

    def kv_send(i):
        which = lax.div(z, last)
        return remote(kw, kvsum.at[which], kf_s.at[i], kf_r.at[which], tp=lax.rem(z + ONE + i, last + ONE))

    def kv_total():
        @pl.when((z == ZERO) | (z == last))
        def _():
            k = first_b
            cs = pl.ds((nb - ONE) * tile, tile)
            far_wait(False, k)
            own_cp = local(own_b.at[:, cs], kw, load.at[ZERO])
            cps = [local(got_b.at[q, :, cs], sb.at[ZERO, q], load.at[ONE + q]) for q in range(THREE)]
            own_cp.start()
            for cp in cps:
                cp.start()
            own_cp.wait()
            for cp in cps:
                cp.wait()
            kw[...] = kw[...] + sb[ZERO, ZERO].astype(F32) + sb[ZERO, ONE].astype(F32) + sb[ZERO, TWO].astype(F32)
            home = local(kw, kvsum.at[lax.div(z, last)], kf_l)
            home.start()
            for i in range(THREE):
                kv_send(i).start()
            home.wait()

        @pl.when((z != ZERO) & (z != last))
        def _():
            far_wait(False, first_b)

    def kv_settle():
        def arrived(which):
            remote(kw, kvsum.at[which], kf_s.at[ZERO], kf_r.at[which], tp=lax.rem(z + ONE, last + ONE)).wait_recv()

        @pl.when(z != ZERO)
        def _():
            arrived(ZERO)

        @pl.when(z != last)
        def _():
            arrived(ONE)

        @pl.when((z == ZERO) | (z == last))
        def _():
            for i in range(THREE):
                kv_send(i).wait_send()

    out_weights().start()
    gv[8:16, :] = jnp.zeros((8, width), F32)
    small = [local(gain, gv.at[pl.ds(ZERO, 8)], load.at[ZERO]), local(wkv, wv, load.at[ONE]), local(table, tv, load.at[TWO])]
    for s in small:
        s.start()

    ctile[:, ZERO:kv] = jnp.zeros((rt_rows, kv), BF16)
    blanks = [local(ctile.at[:, pl.ds(ZERO, kv)], dcat.at[pl.ds(i * rt_rows, rt_rows), pl.ds(kb, kv)], wload.at[TWO + i])
              for i in range(nc // TWO)]
    for s in blanks:
        s.start()
    for s in blanks + small:
        s.wait()

    steps = nc // TWO
    a_at, h_at, b_at = steps, steps + 4, TWO * steps + 4
    kv_at = b_at + 10
    per_a, per_b = -(-na // TWO), -(-first_b // TWO)

    def share(at, lo, hi, per, i):
        return jnp.minimum(lo + i * per, hi), jnp.minimum(lo + (i + ONE) * per, hi)

    def phase(s, at, n):
        return pl.when((s >= at) & (s < at + n))

    def step(s, carry):
        slot(s - ONE)

        @phase(s, ZERO, steps)
        def _():
            @pl.when(s == ZERO)
            def _():
                out_weights().wait()
                in_weights().start()

            y_step(s)

        @phase(s, a_at, TWO)
        def _():
            @pl.when(s == a_at)
            def _():
                operand(dy)

            odd_steps(True, *share(s, ZERO, na, per_a, s - a_at), (ZERO, na))

        @phase(s, a_at + TWO, TWO)
        def _():
            even_steps(True, *share(s, ZERO, na, per_a, s - (a_at + TWO)), (ZERO, na))

        @phase(s, h_at, steps)
        def _():
            @pl.when(s == h_at)
            def _():
                in_weights().wait()

            h_step(s - h_at)

        for part_b in range(TWO):
            lo, hi = (ZERO, first_b) if part_b == ZERO else (first_b, nb)
            at = b_at + 4 * part_b

            @phase(s, at, TWO)
            def _():
                if part_b == ZERO:
                    @pl.when(s == at)
                    def _():
                        operand(h)

                odd_steps(False, *share(s, lo, hi, per_b, s - at), (lo, hi))

            @phase(s, at + TWO, TWO)
            def _():
                even_steps(False, *share(s, lo, hi, per_b, s - (at + TWO)), (lo, hi))

        @pl.when(s == kv_at)
        def _():
            kv_total()

        @pl.when(s == TWO * nc + hop_lag * last)
        def _():
            gain_total()

        return carry

    lax.fori_loop(ZERO, end + TWO, step, ZERO)
    far_waits(True)
    far_waits(False, first_b)
    kv_settle()


def back_call(att, act, wod, gate, up, dact, dq, wcat, wkv, dkv, table, h, dy, x, gain, nc=12, col=1024, tile=512):
    tok, width = h.shape
    inner, ff = att.shape[1], act.shape[1]
    ka, kb, kv = inner + ff, wcat.shape[1], dkv.shape[1]
    cr = tok // (2 * nc)
    rt_rows = 4 * cr
    blk, mid = width // 8, width // 2
    na, nb = ka // tile, (kb + kv) // tile
    big = max(mid, 2 * tile)
    shape = jax.ShapeDtypeStruct
    outs = (
        shape((tok, width), BF16), shape((tok, width), BF16), shape((2, tok, width), BF16), shape((2, 2 * nc, cr, width), BF16),
        shape((2, nc, cr, kv), BF16), shape((tok, kb + kv), BF16), shape((nc * cr, width), F32),
        shape((ka, mid), F32), shape((mid, kb + kv), F32), shape((ka, blk), F32), shape((blk, kb + kv), F32),
        shape((3, ka, blk), WIRE), shape((3, blk, kb + kv), WIRE), shape((2, 8, blk), F32), shape((8, 8, blk), F32), shape((2, blk, kv), F32),
        shape((3, ka, blk), WIRE), shape((3, blk, kb + kv), WIRE),
    )
    sems = pltpu.SemaphoreType.DMA
    scratch = [
        pltpu.VMEM((max(ka, tok), width), BF16), pltpu.VMEM((width, kb), BF16), pltpu.VMEM((2, tok, tile), BF16),
        pltpu.VMEM((width, kv), BF16), pltpu.VMEM(table.shape, F32),
        pltpu.VMEM((rt_rows, max(ka, kb)), BF16), pltpu.VMEM((rt_rows, max(ff, width)), BF16),
        pltpu.VMEM((big, big), F32), pltpu.VMEM((mid, tile), F32),
        pltpu.VMEM((2, 3, tile, blk), WIRE), pltpu.VMEM((2, 3, blk, tile), WIRE),
        pltpu.VMEM((2, cr, width), BF16), pltpu.VMEM((2, cr, width), BF16), pltpu.VMEM((2, 3, cr, width), BF16),
        pltpu.VMEM((cr, width), BF16), pltpu.VMEM((cr, width), BF16), pltpu.VMEM((cr, width), F32),
        pltpu.VMEM((2, cr, kv), BF16), pltpu.VMEM((2, cr, kv), BF16), pltpu.VMEM((2, 3, cr, kv), BF16),
        pltpu.VMEM((16, width), F32), pltpu.VMEM((blk, kv), F32), pltpu.VMEM((8, 8, blk), F32),
        sems((5,)), sems((11,)), sems, sems((2, 7)), sems((2, 3)), sems((2,)),
        sems((2, 2 * nc)), sems((2, 2 * nc)), sems((2, nc)), sems((2, nc)), sems((2, 2 * nc)), sems((2, 2 * nc)),
        sems((na + nb,)), sems((na + nb,)), sems((3, na + nb)), sems((3, na + nb)), sems((2 + mid // tile,)), sems((2, 3)),
        sems((3,)), sems((2,)), sems, sems((8,)), sems((8,)), sems((8,)), sems((3,)), sems((2,)),
    ]
    flops = 2 * tok * width * (2 * ka + 2 * kb)
    anywhere = pl.BlockSpec(memory_space=pl.ANY)
    return pl.pallas_call(
        functools.partial(back_kernel, (nc, cr, col, tile)),
        out_shape=outs,
        in_specs=[anywhere] * 15,
        out_specs=tuple(anywhere for _ in outs),
        scratch_shapes=scratch,
        cost_estimate=pl.CostEstimate(flops=2 * flops, bytes_accessed=200_000_000, transcendentals=tok * ff),
        compiler_params=pltpu.CompilerParams(vmem_limit_bytes=67_000_000, has_side_effects=True),
        name='backward',
    )(att, act, wod, gate, up, dact, dq, wcat, wkv, dkv, table, h, dy, x, gain)


def attention_kernel(heads, qkv, datt, table, att, dq, dkv, krot, dk_acc, dv_acc):
    n_pos = qkv.shape[0]
    head = qkv.shape[1] // (heads + 2)
    half = head // 2
    scale = 1.0 / math.sqrt(head)
    qb = 256

    def cos_of(sl):
        return table[sl, 0:half], table[sl, half:head]

    def turn(lo, sl, factor):
        cos_t, sin_t = cos_of(sl)
        first = qkv[sl, lo:lo + half].astype(F32)
        second = qkv[sl, lo + half:lo + head].astype(F32)
        return jnp.concatenate([(first * cos_t - second * sin_t) * factor, (second * cos_t + first * sin_t) * factor], axis=-1).astype(BF16)

    k_at, v_at = heads * head, (heads + 1) * head
    krot[...] = turn(k_at, slice(0, n_pos), 1.0)
    dk_acc[...] = jnp.zeros_like(dk_acc)
    dv_acc[...] = jnp.zeros_like(dv_acc)
    for r in range(heads):
        for i in range(n_pos // qb):
            sl = slice(i * qb, (i + 1) * qb)
            upto = (i + 1) * qb
            q = turn(r * head, sl, scale)
            k = krot[0:upto, :]
            v = qkv[0:upto, v_at:v_at + head]
            scores = contract(q, k, (1, 1))
            rows = lax.broadcasted_iota(jnp.int32, (qb, upto), 0) + i * qb
            scores = jnp.where(rows >= lax.broadcasted_iota(jnp.int32, (qb, upto), 1), scores, -1e30)
            exp_val = jnp.exp(scores - jnp.max(scores, axis=-1, keepdims=True))
            prob = exp_val / jnp.sum(exp_val, axis=-1, keepdims=True)
            prob_b = prob.astype(BF16)
            att[sl, r * head:(r + 1) * head] = contract(prob_b, v, (1, 0)).astype(BF16)
            do = datt[sl, r * head:(r + 1) * head]
            d_prob = contract(do, v, (1, 1)).astype(BF16).astype(F32)
            d_scores = (prob * (d_prob - jnp.sum(d_prob * prob, axis=-1, keepdims=True))).astype(BF16)
            d_rot = contract(d_scores, k, (1, 0)).astype(BF16).astype(F32) * scale
            cos_t, sin_t = cos_of(sl)
            first, second = d_rot[:, 0:half], d_rot[:, half:head]
            dq[sl, r * head:r * head + half] = (first * cos_t + second * sin_t).astype(BF16)
            dq[sl, r * head + half:(r + 1) * head] = (second * cos_t - first * sin_t).astype(BF16)
            dk_acc[0:upto, :] += contract(d_scores, q, (0, 0))
            dv_acc[0:upto, :] += contract(prob_b, do, (0, 0))
    dkv[:, 0:head] = dk_acc[...].astype(BF16)
    dkv[:, head:2 * head] = dv_acc[...].astype(BF16)


def attention_call(qkv, datt, table, n_batch):
    tok, wide = qkv.shape
    inner = datt.shape[1]
    head = table.shape[1]
    n_pos = tok // n_batch
    heads = inner // head

    def rows(n):
        return pl.BlockSpec((n_pos, n), lambda b: (b, 0))

    shape = jax.ShapeDtypeStruct
    flops = 2 * n_batch * heads * n_pos * n_pos * head * 7
    return pl.pallas_call(
        functools.partial(attention_kernel, heads),
        grid=(n_batch,),
        out_shape=(shape((tok, inner), BF16), shape((tok, inner), BF16), shape((tok, 2 * head), BF16)),
        in_specs=[rows(wide), rows(inner), pl.BlockSpec(table.shape, lambda b: (0, 0))],
        out_specs=(rows(inner), rows(inner), rows(2 * head)),
        scratch_shapes=[pltpu.VMEM((n_pos, head), BF16), pltpu.VMEM((n_pos, head), F32), pltpu.VMEM((n_pos, head), F32)],
        cost_estimate=pl.CostEstimate(flops=flops, bytes_accessed=20_000_000, transcendentals=n_batch * heads * n_pos * n_pos),
        compiler_params=pltpu.CompilerParams(vmem_limit_bytes=67_000_000),
        name='attention',
    )(qkv, datt, table)


def finish_kernel(y, gx, own_o, own_d, got_o, got_d, own_b, got_b, kvs, y_out, gx_out, o_out, d_out, g_out, u_out, q_out, k_out, v_out):
    y_out[...] = y[...]
    gx_out[...] = gx[...]

    def total(own, got):
        return own[...] + got[0].astype(F32) + got[1].astype(F32) + got[2].astype(F32)

    o_out[...] = total(own_o, got_o)
    d_out[...] = total(own_d, got_d)
    ff, inner, head = g_out.shape[1], q_out.shape[1], k_out.shape[1]
    at = 0
    for out in (g_out, u_out, q_out):
        cols = slice(at, at + out.shape[1])
        out[...] = own_b[:, cols] + got_b[0, :, cols].astype(F32) + got_b[1, :, cols].astype(F32) + got_b[2, :, cols].astype(F32)
        at += out.shape[1]
    k_out[...] = kvs[0, :, 0:head] + kvs[1, :, 0:head]
    v_out[...] = kvs[0, :, head:] + kvs[1, :, head:]


def finish_call(y, gx, own_a, got_a, own_b, got_b, kvs, inner, ff, steps=16):
    tok, width = y.shape
    blk, wide = own_b.shape
    kv = kvs.shape[2]
    skip = inner // (ff // steps)
    shape = jax.ShapeDtypeStruct

    def rows(n, cols, off=0):
        return pl.BlockSpec((n // steps, cols), lambda i: (i + off, 0))

    def three(n, cols, off=0):
        return pl.BlockSpec((3, n // steps, cols), lambda i: (0, i + off, 0))

    used = 2 * ff + inner
    return pl.pallas_call(
        finish_kernel,
        grid=(steps,),
        out_shape=(shape((tok, width), BF16), shape((tok, width), BF16), shape((inner, blk), F32), shape((ff, blk), F32),
                   shape((blk, ff), F32), shape((blk, ff), F32), shape((blk, inner), F32), shape((blk, kv // 2), F32), shape((blk, kv // 2), F32)),
        in_specs=[rows(tok, width), rows(tok, width), rows(inner, blk), rows(ff, blk, skip), three(inner, blk), three(ff, blk, skip),
                  rows(blk, used), three(blk, used), pl.BlockSpec((2, blk // steps, kv), lambda i: (0, i, 0))],
        out_specs=(rows(tok, width), rows(tok, width), rows(inner, blk), rows(ff, blk), rows(blk, ff), rows(blk, ff), rows(blk, inner),
                   rows(blk, kv // 2), rows(blk, kv // 2)),
        cost_estimate=pl.CostEstimate(flops=8 * blk * wide, bytes_accessed=66_000_000, transcendentals=0),
        compiler_params=pltpu.CompilerParams(vmem_limit_bytes=67_000_000),
        name='finish',
    )(y, gx, own_a, own_a, got_a, got_a, own_b, got_b, kvs)


def solution(mesh):
    def device_step(x_in, dy_out, ln_gain, w_q, w_k, w_v, w_o, w_gate, w_up, w_down):
        n_batch, seq_len, width = x_in.shape
        head_dim = w_k.shape[1]
        inner = w_q.shape[1]
        ff = w_gate.shape[1]
        tok = n_batch * seq_len
        x_rows = x_in.reshape(tok, width)
        dy = dy_out.reshape(tok, width)
        table = jnp.concatenate(rope_tables(seq_len, head_dim), axis=-1)

        gain8 = jnp.broadcast_to(ln_gain[None, :], (8, ln_gain.shape[0]))
        front = front_call(x_rows, dy, gain8, (w_q, w_k, w_v, w_o, w_down, w_gate, w_up))
        wcat, wkv, wod, gain, h_norm, qkv, gate, up, act, d_att, d_act = front
        att, d_q, dkv = attention_call(qkv, d_att, table, n_batch)
        res = back_call(att, act, wod, gate, up, d_act, d_q, wcat, wkv, dkv, table, h_norm, dy, x_rows, gain)
        own_a, own_b, got_a, got_b, gsum, _, kvsum = res[9:16]
        done = finish_call(res[0], res[1], own_a, got_a, own_b, got_b, kvsum, inner, ff)
        y_rows, gx_rows, grad_wo, grad_wdown, grad_wgate, grad_wup, grad_wq, grad_wk, grad_wv = done
        grad_gain = gsum[0, 0] + gsum[1, 0]
        return (y_rows.reshape(x_in.shape), gx_rows.reshape(x_in.shape), grad_gain, grad_wq, grad_wk, grad_wv,
                grad_wo, grad_wgate, grad_wup, grad_wdown)

    act_spec = P('fsdp', None, None)
    row_spec = P('fsdp', 'tp')
    kv_spec = P('fsdp', None)
    col_spec = P('tp', 'fsdp')
    in_specs = (act_spec, act_spec, P('fsdp'), row_spec, kv_spec, kv_spec, col_spec, row_spec, row_spec, col_spec)
    out_specs = (act_spec, act_spec, P('fsdp'), row_spec, kv_spec, kv_spec, col_spec, row_spec, row_spec, col_spec)
    return jax.shard_map(device_step, mesh=mesh, in_specs=in_specs, out_specs=out_specs, check_vma=False)
```
